32 devices in a mesh: box: 4 (over z), dir: 8 (over y, x, core).
Axes of the slice: x: 2, y: 2, z: 4, core: 2. Of those that a mesh axis runs over, the one named last changes fastest.
Arguments:
- currents: bfloat16 [4096, 256, 128], P(('box', 'dir')), may hold values from -6 to 6
- leaf_parent: int32 [4096], P(('box', 'dir')), may hold values from 0 to 63, as said below
- near_links: int32 [4096, 2], P(('box', 'dir')), may hold values 0 or 1
- near_blocks: bfloat16 [3, 256, 256], replicated, may hold values from -0.375 to 0.375
- aggregate_maps: bfloat16 [64, 256, 256], replicated, may hold values from -0.375 to 0.375
- far_boxes: int32 [64, 64], P('box'), may hold values from 0 to 63
- far_counts: int32 [64], P('box'), may hold values from 16 to 64
- translate_coef: float32 [64, 64, 256], P('box'), may hold values from 0.005 to 0.05
- time_kernel: float32 [128], replicated, may hold values from -0.5 to 0.5
- disaggregate_maps: bfloat16 [64, 256, 256], replicated, may hold values from -0.375 to 0.375
Outputs:
- field: bfloat16 [4096, 256, 128], P(('box', 'dir'))
The draws below stay inside these ranges and needn't reach their ends.
Inputs may be any that keep to these rules, and one draw needn't show every extreme that they name: `leaf_parent`: the leaves k * 64 to (k + 1) * 64 - 1 share one parent. The leaves g * 1024 to (g + 1) * 1024 - 1 have as parents the top-level boxes g * 16 to (g + 1) * 16 - 1, each exactly once as a run.
All inputs are finite; a program needn't handle non-finite values. No bound on the sum of `near_links` on one device may be relied on, other than what follows from the above.
Results may differ from the reference program's by a relative error of at most 0.0047.
Values may be sent and summed in bfloat16 or wider, within the bound.
A program may use at most 192 MiB of HBM per device.

```python
import math
import jax
import jax.numpy as jnp
from jax import lax

P_SIZE = 256
K_TOP = 256
S = 128
LEAF_TOP = 64
FAR = 64
LEAVES = 4096
GROUP_LEAVES = 1024
TOP_DEV = 16
TOPS = 64


def draw_leaf_parent(key, part):
    group_count = LEAVES // GROUP_LEAVES
    group_keys = jax.random.split(jax.random.fold_in(key, 11), group_count)
    orders = jax.vmap(lambda k: jax.random.permutation(k, TOP_DEV))(group_keys).astype(jnp.int32)
    leaf_index = jnp.arange(LEAVES, dtype=jnp.int32)
    group = leaf_index // GROUP_LEAVES
    run_index = leaf_index % GROUP_LEAVES // LEAF_TOP
    return (group * TOP_DEV + orders[group, run_index]).astype(jnp.int32)


def set_ends(entries, key, low, high):
    spot = [jax.random.randint(jax.random.fold_in(key, axis), (), 0, length) for axis, length in enumerate(entries.shape)]
    widest = entries.shape.index(max(entries.shape))
    beside = spot[:widest] + [(spot[widest] + 1) % entries.shape[widest]] + spot[widest + 1:]
    return entries.at[tuple(spot)].set(low).at[tuple(beside)].set(high)


def level_of(stream_key, shape, shards, smallest, top_value):
    def one(axis_at, shards_of):
        draws = jax.random.uniform(jax.random.fold_in(jax.random.fold_in(stream_key, 6), axis_at), (shards_of,), jnp.float32, smallest / len(shards), top_value / len(shards))
        return jnp.repeat(jnp.exp(draws), shape[axis_at] // shards_of).reshape((-1,) + (1,) * (len(shape) - axis_at - 1))

    level = one(*shards[0])
    for cut in shards[1:]:
        level = level * one(*cut)
    return level


def bell_draw(own_key, dims, deviation, bound, cuts=(), kind=jnp.bfloat16):
    values = deviation * jax.random.normal(own_key, dims, jnp.float32)
    if cuts:
        values = values * level_of(own_key, dims, cuts, -0.22, 0.18)
    return jnp.clip(values, -bound, bound).astype(kind)


def setup_inputs(seed: int = 0) -> dict:
    key_of = jax.random.split(jax.random.key(seed), 11)
    currents = bell_draw(key_of[0], (LEAVES, P_SIZE, S), 1.0, 6.0, ((0, 32),))
    leaf_parent = draw_leaf_parent(jax.random.fold_in(key_of[10], 71), 0)
    near_links = set_ends((jax.random.randint(key_of[2], (LEAVES, 2), 0, 4) < 3).astype(jnp.int32), jax.random.fold_in(key_of[2], 1), 0, 1)
    near_blocks = bell_draw(key_of[3], (3, P_SIZE, P_SIZE), P_SIZE ** -0.5, 0.375)
    aggregate_maps = bell_draw(key_of[4], (LEAF_TOP, K_TOP, P_SIZE), P_SIZE ** -0.5, 0.375)
    far_boxes = set_ends(jax.random.randint(key_of[5], (TOPS, FAR), 0, TOPS), jax.random.fold_in(key_of[5], 1), 0, TOPS - 1).astype(jnp.int32)
    far_counts = set_ends(jax.random.randint(key_of[6], (TOPS,), FAR // 4, FAR + 1), jax.random.fold_in(key_of[6], 1), FAR // 4, FAR).astype(jnp.int32)
    translate_coef = jnp.clip(jnp.exp(math.log(0.05) - 2.3025851 * jax.random.uniform(key_of[7], (TOPS, FAR, K_TOP), jnp.float32) ** level_of(key_of[7], (TOPS, FAR, K_TOP), ((0, 4),), -0.2, 0.2)), 0.005, 0.05)
    time_kernel = bell_draw(key_of[8], (S,), S ** -0.5, 0.5, (), jnp.float32)
    disaggregate_maps = bell_draw(key_of[9], (LEAF_TOP, P_SIZE, K_TOP), K_TOP ** -0.5, 0.375)
    return dict(currents=currents, leaf_parent=leaf_parent, near_links=near_links, near_blocks=near_blocks, aggregate_maps=aggregate_maps, far_boxes=far_boxes, far_counts=far_counts, translate_coef=translate_coef, time_kernel=time_kernel, disaggregate_maps=disaggregate_maps)


def time_matrix(kernel):
    sample_lag = jnp.arange(S)[:, None] - jnp.arange(S)[None, :]
    return jnp.where(sample_lag >= 0, kernel[jnp.clip(sample_lag, 0, S - 1)], jnp.zeros((), kernel.dtype))


def reference(currents, leaf_parent, near_links, near_blocks, aggregate_maps, far_boxes, far_counts, translate_coef, time_kernel, disaggregate_maps):
    highest = lax.Precision.HIGHEST
    blocks = LEAVES // 8
    agg_float = aggregate_maps.astype(jnp.float32)
    cur_blocks = currents.reshape(blocks, 8, P_SIZE, S)
    par_blocks = leaf_parent.reshape(blocks, 8)
    block_ids = jnp.arange(blocks, dtype=jnp.int32)

    def add_block(running, inputs):
        block_cur, block_par, block_id = inputs
        first_map = ((block_id * 8) % LEAF_TOP).astype(jnp.int32)
        map_block = lax.dynamic_slice_in_dim(agg_float, first_map, 8, 0)
        ray_terms = jnp.einsum('sqp,spt->sqt', map_block, block_cur.astype(jnp.float32), precision=highest)
        return running.at[block_par].add(ray_terms), None

    top_rays, _ = lax.scan(add_block, jnp.zeros((TOPS, K_TOP, S), jnp.float32), (cur_blocks, par_blocks, block_ids))
    top_rays = top_rays.astype(jnp.bfloat16)
    is_valid = (jnp.arange(FAR)[None, :] < far_counts[:, None]).astype(jnp.float32)
    matches = (far_boxes[:, :, None] == jnp.arange(TOPS)[None, None, :]).astype(jnp.float32) * is_valid[:, :, None]
    weights = jnp.einsum('cfs,cfq->csq', matches, translate_coef, precision=highest)
    far_sum = jnp.einsum('csq,sqt->cqt', weights, top_rays.astype(jnp.float32), precision=highest)
    incoming = jnp.einsum('cqs,ts->cqt', far_sum, time_matrix(time_kernel), precision=highest).astype(jnp.bfloat16)
    incoming_float = incoming.astype(jnp.float32)
    zero_leaf = jnp.zeros((1, P_SIZE, S), currents.dtype)
    padded = jnp.concatenate([zero_leaf, currents, zero_leaf], axis=0)
    near_float = near_blocks.astype(jnp.float32)
    dis_float = disaggregate_maps.astype(jnp.float32)

    def leaf_block(block_index):
        first_leaf = (block_index * 8).astype(jnp.int32)
        first_map = (first_leaf % LEAF_TOP).astype(jnp.int32)
        before_leaf = lax.dynamic_slice_in_dim(padded, first_leaf, 8, 0).astype(jnp.float32)
        middle_leaf = lax.dynamic_slice_in_dim(padded, first_leaf + 1, 8, 0).astype(jnp.float32)
        after_leaf = lax.dynamic_slice_in_dim(padded, first_leaf + 2, 8, 0).astype(jnp.float32)
        link_mask = lax.dynamic_slice_in_dim(near_links, first_leaf, 8, 0).astype(jnp.float32)
        parents = lax.dynamic_slice_in_dim(leaf_parent, first_leaf, 8, 0)
        map_block = lax.dynamic_slice_in_dim(dis_float, first_map, 8, 0)
        near_field = jnp.einsum('pr,srt->spt', near_float[0], middle_leaf, precision=highest)
        near_field = near_field + link_mask[:, 0, None, None] * jnp.einsum('pr,srt->spt', near_float[1], before_leaf, precision=highest)
        near_field = near_field + link_mask[:, 1, None, None] * jnp.einsum('pr,srt->spt', near_float[2], after_leaf, precision=highest)
        far_field = jnp.einsum('spq,sqt->spt', map_block, incoming_float[parents], precision=highest)
        return (near_field + far_field).astype(jnp.bfloat16)

    field_out = lax.map(leaf_block, jnp.arange(blocks, dtype=jnp.int32))
    return field_out.reshape(LEAVES, P_SIZE, S)
```

```python
import functools
import jax
import jax.numpy as jnp
from jax import lax
from jax.experimental import pallas as pl
from jax.experimental.pallas import tpu as pltpu
from jax.sharding import PartitionSpec as P

MESH = pl.DeviceIdType.MESH
HIGHEST = lax.Precision.HIGHEST
F32 = jnp.float32
BF16 = jnp.bfloat16
AGG_CHUNK = 4
NEAR_UNROLL = 2


def split_high_low(value):
    high = value.astype(BF16)
    return high, (value - high.astype(F32)).astype(BF16)


def rays_kernel(
    boxes,
    dirs,
    runs,
    cur_hbm,
    agg_hbm,
    dis_hbm,
    coef_hbm,
    blocks_ref,
    links_ref,
    leaf_parent_ref,
    lists_ref,
    counts_ref,
    kernel_ref,
    incoming_ref,
    near_ref,
    dis_ref,
    leaf,
    acc,
    rays,
    rays_all,
    parent_row_ref,
    parent_all,
    coef,
    wide_ref,
    weights_ref,
    split_ref,
    spread_ref,
    far_ref,
    time_ref,
    stage_ref,
    landed,
    agg_sem,
    cur_sem,
    coef_sem,
    dis_sem,
    par_send,
    par_recv,
    ray_send,
    ray_recv,
    back_send,
    back_recv,
    rim_send,
    rim_recv,
):
    my_box = lax.axis_index("box")
    my_dir = lax.axis_index("dir")
    me = my_box * dirs + my_dir
    devices = boxes * dirs
    leaf_top = agg_hbm.shape[0]
    samples = cur_hbm.shape[-1]
    directions = agg_hbm.shape[1]
    rows = directions // dirs
    top_local = counts_ref.shape[0]
    slots = lists_ref.shape[1]
    width = parent_row_ref.shape[-1]
    places = dirs * runs
    plane = places * rows
    leaves = runs * leaf_top
    peers = [(kb, kd) for kb in range(boxes) for kd in range(dirs) if kb or kd]
    peers.sort(key=lambda p: -min(p[0], boxes - p[0]))

    def target(kb, kd):
        return lax.rem(my_box + kb, boxes), lax.rem(my_dir + kd, dirs)

    barrier = pltpu.get_barrier_semaphore()
    for kb, kd in peers:
        tb, td = target(kb, kd)
        pl.semaphore_signal(
            barrier, inc=1, device_id={"box": tb, "dir": td}, device_id_type=MESH
        )

    chunks = leaf_top // AGG_CHUNK

    def loads(c):
        first = c * AGG_CHUNK
        out = [
            pltpu.make_async_copy(
                agg_hbm.at[pl.ds(first, AGG_CHUNK)],
                dis_ref.at[pl.ds(first, AGG_CHUNK)],
                agg_sem.at[c],
            )
        ]
        for j in range(runs):
            at = j * leaf_top + first
            out.append(
                pltpu.make_async_copy(
                    cur_hbm.at[pl.ds(at, AGG_CHUNK)],
                    leaf.at[pl.ds(at + 1, AGG_CHUNK)],
                    cur_sem.at[j, c],
                )
            )
        return out

    def start_loads(c, carry):
        for copy in loads(c):
            copy.start()
        return carry

    lax.fori_loop(0, chunks, start_loads, 0)
    block_at = my_dir * rows
    lane_tile = lax.div(block_at, 128) * 128
    coef_copy = pltpu.make_async_copy(
        coef_hbm.at[:, :, pl.ds(pl.multiple_of(lane_tile, 128), 128)], coef, coef_sem
    )
    coef_copy.start()

    @pl.when(me == 0)
    def _():
        leaf[0] = jnp.zeros(leaf.shape[1:], BF16)

    @pl.when(me == devices - 1)
    def _():
        leaf[leaves + 1] = jnp.zeros(leaf.shape[1:], BF16)

    lane = lax.broadcasted_iota(jnp.int32, (1, width), 1)
    spare = jnp.where(me == 0, -1, 0)
    parent_row = jnp.where(lane >= devices * runs, spare, jnp.zeros((1, width), jnp.int32))
    for j in range(runs):
        parent_row = jnp.where(lane == me * runs + j, leaf_parent_ref[j * leaf_top], parent_row)
    parent_row_ref[...] = parent_row.astype(F32)
    acc[...] = jnp.zeros_like(acc)

    def aggregate(c, carry):
        for copy in loads(c):
            copy.wait()
        first = c * AGG_CHUNK
        maps = jnp.concatenate([dis_ref[first + i] for i in range(AGG_CHUNK)], axis=1)
        held = jnp.concatenate(
            [
                jnp.concatenate([leaf[1 + j * leaf_top + first + i] for j in range(runs)], axis=1)
                for i in range(AGG_CHUNK)
            ],
            axis=0,
        )
        acc[...] += jnp.dot(maps, held, preferred_element_type=F32)
        return carry

    lax.fori_loop(0, chunks // 2, aggregate, 0)

    pl.semaphore_wait(barrier, len(peers))

    def parent_copy(kb, kd):
        tb, td = target(kb, kd)
        return pltpu.make_async_remote_copy(
            src_ref=parent_row_ref,
            dst_ref=parent_all.at[me],
            send_sem=par_send.at[tb * dirs + td],
            recv_sem=par_recv.at[me],
            device_id={"box": tb, "dir": td},
            device_id_type=MESH,
        )

    def ray_copy(kb, kd):
        tb, td = target(kb, kd)
        block = pl.ds(pl.multiple_of(td * rows, rows), rows)
        return pltpu.make_async_remote_copy(
            src_ref=rays.at[:, block, :],
            dst_ref=rays_all.at[my_box, my_dir],
            send_sem=ray_send.at[tb * dirs + td],
            recv_sem=ray_recv.at[me],
            device_id={"box": tb, "dir": td},
            device_id_type=MESH,
        )

    def rim_copy(side):
        other = lax.rem(me + (1 if side == 0 else devices - 1), devices)
        return pltpu.make_async_remote_copy(
            src_ref=cur_hbm.at[leaves - 1 if side == 0 else 0],
            dst_ref=leaf.at[0 if side == 0 else leaves + 1],
            send_sem=rim_send.at[side],
            recv_sem=rim_recv.at[side],
            device_id={"box": lax.div(other, dirs), "dir": lax.rem(other, dirs)},
            device_id_type=MESH,
        )

    for kb, kd in peers:
        parent_copy(kb, kd).start()

    @pl.when(me < devices - 1)
    def _():
        rim_copy(0).start()

    @pl.when(me > 0)
    def _():
        rim_copy(1).start()

    parent_all[me] = parent_row_ref[...]

    lax.fori_loop(chunks // 2, chunks, aggregate, 0)

    for j in range(runs):
        rays[j] = acc[:, j * samples : (j + 1) * samples].astype(BF16)
    for kb, kd in peers:
        ray_copy(kb, kd).start()
    own = pl.ds(pl.multiple_of(block_at, rows), rows)
    rays_all[my_box, my_dir] = rays[:, own, :]
    dis_copy = pltpu.make_async_copy(dis_hbm, dis_ref, dis_sem)
    dis_copy.start()

    @pl.when(me < devices - 1)
    def _():
        rim_copy(0).wait_send()
        rim_copy(1).wait_recv()

    @pl.when(me > 0)
    def _():
        rim_copy(1).wait_send()
        rim_copy(0).wait_recv()

    def near_step(step, carry):
        blocks = jnp.concatenate([blocks_ref[k] for k in range(3)], axis=1)
        for u in range(NEAR_UNROLL):
            at = step * NEAR_UNROLL + u
            parts = [[], [], []]
            for j in range(runs):
                row = j * leaf_top + at
                low = leaf[row]
                high = leaf[row + 2]
                parts[0].append(leaf[row + 1])
                parts[1].append(jnp.where(links_ref[0, row] != 0, low, jnp.zeros_like(low)))
                parts[2].append(jnp.where(links_ref[1, row] != 0, high, jnp.zeros_like(high)))
            held = jnp.concatenate([jnp.concatenate(p, axis=1) for p in parts], axis=0)
            total = jnp.dot(blocks, held, preferred_element_type=F32)
            for j in range(runs):
                near_ref[j, at] = total[:, j * samples : (j + 1) * samples].astype(BF16)
        return carry

    lax.fori_loop(0, leaf_top // NEAR_UNROLL, near_step, 0)

    lag = lax.broadcasted_iota(jnp.int32, (samples, samples), 1) - lax.broadcasted_iota(
        jnp.int32, (samples, samples), 0
    )

    def add_lag(i, matrix):
        return jnp.where(lag == i, kernel_ref[i], matrix)

    time_matrix = lax.fori_loop(0, samples, add_lag, jnp.zeros((samples, samples), F32))
    time_high, time_low = split_high_low(time_matrix)
    time_ref[:samples, :samples] = time_high
    time_ref[:samples, samples:] = time_low
    time_ref[samples:, :samples] = time_high
    time_ref[samples:, samples:] = jnp.zeros_like(time_low)

    def arrived(ref, send_sem, recv_sem):
        pltpu.make_async_remote_copy(
            src_ref=ref,
            dst_ref=ref,
            send_sem=send_sem,
            recv_sem=recv_sem,
            device_id={"box": my_box, "dir": lax.rem(my_dir + 1, dirs)},
            device_id_type=MESH,
        ).wait_recv()

    for kb, kd in peers:
        sb, sd = target(kb, kd)
        slot = sb * dirs + sd
        arrived(parent_all.at[slot], par_send.at[slot], par_recv.at[slot])
    parents = jnp.zeros((1, width), F32)
    for slot in range(devices):
        parents = parents + parent_all[slot]
    column = jnp.broadcast_to(parents, (128, width)).T[:, :slots]
    spot = lax.broadcasted_iota(jnp.int32, (1, slots), 1)
    coef_copy.wait()
    inside = pl.ds(pl.multiple_of(block_at - lane_tile, rows), rows)
    for c in range(top_local):
        used = jnp.where(spot < counts_ref[c], lists_ref[c : c + 1, :], -2)
        match = (column == used.astype(F32)).astype(F32)
        wide_ref[c] = lax.dot_general(
            coef[c],
            match,
            (((0,), (1,)), ((), ())),
            preferred_element_type=F32,
            precision=HIGHEST,
        )
        weights_ref[c] = wide_ref[c, inside, :]
    first_top = my_box * top_local
    for place in range(places):
        at = my_box * places + place
        parent = jnp.sum(jnp.where(lane == at, parents, 0.0), axis=1, keepdims=True)
        chosen = jnp.zeros((rows, width), F32)
        for c in range(top_local):
            hit = parent == (first_top + c).astype(F32)
            chosen = jnp.where(hit, weights_ref[c], chosen)
        high, low = split_high_low(chosen)
        split_ref[place * rows : (place + 1) * rows, :] = high
        split_ref[plane + place * rows : plane + (place + 1) * rows, :] = low

    part = 256

    def spread(b, carry):
        for k in range(plane // part):
            spot_k = k * part + lax.broadcasted_iota(jnp.int32, (width, part), 1)
            owner = b * places + lax.div(spot_k, rows)
            pick = (owner == lax.broadcasted_iota(jnp.int32, (width, part), 0)).astype(F32)
            wide = jnp.dot(split_ref[...], pick.astype(BF16), preferred_element_type=F32)
            row_q = lax.rem(lax.broadcasted_iota(jnp.int32, (2 * plane, part), 0), rows)
            lane_q = lax.rem(lax.broadcasted_iota(jnp.int32, (2 * plane, part), 1), rows)
            spread_ref[b, :, k * part : (k + 1) * part] = jnp.where(
                row_q == lane_q, wide, 0.0
            ).astype(BF16)
        return carry

    lax.fori_loop(0, boxes, spread, 0)

    order = sorted(range(boxes), key=lambda kb: min(kb, boxes - kb))
    for n, kb in enumerate(order):
        sb = lax.rem(my_box + kb, boxes)
        for kd in range(dirs):
            if kb or kd:
                sd = lax.rem(my_dir + kd, dirs)
                slot = sb * dirs + sd
                arrived(rays_all.at[sb, sd], ray_send.at[slot], ray_recv.at[slot])
        held = rays_all[sb].reshape(plane, samples)
        part_sum = jnp.dot(spread_ref[sb], held, preferred_element_type=F32)
        if n == 0:
            far_ref[...] = part_sum
        else:
            far_ref[...] += part_sum

    far_high, far_low = split_high_low(far_ref[:plane, :] + far_ref[plane:, :])
    both = jnp.dot(
        jnp.concatenate([far_high, far_low], axis=1), time_ref[...], preferred_element_type=F32
    )
    incoming = (both[:, :samples] + both[:, samples:]).astype(BF16)
    for d in range(dirs):
        for j in range(runs):
            place = d * runs + j
            stage_ref[d, :, j * samples : (j + 1) * samples] = incoming[
                place * rows : (place + 1) * rows, :
            ]

    def back_copy(kd):
        td = lax.rem(my_dir + kd, dirs)
        return pltpu.make_async_remote_copy(
            src_ref=stage_ref.at[td],
            dst_ref=landed.at[my_dir],
            send_sem=back_send.at[td],
            recv_sem=back_recv.at[my_dir],
            device_id={"box": my_box, "dir": td},
            device_id_type=MESH,
        )

    for kd in range(1, dirs):
        back_copy(kd).start()
    landed[my_dir] = stage_ref[my_dir]
    for kb, kd in peers:
        parent_copy(kb, kd).wait_send()
        ray_copy(kb, kd).wait_send()
    dis_copy.wait()
    for kd in range(1, dirs):
        sd = lax.rem(my_dir + kd, dirs)
        arrived(landed.at[sd], back_send.at[sd], back_recv.at[sd])
    incoming_ref[...] = landed[...].reshape(directions, runs * samples)
    for kd in range(1, dirs):
        back_copy(kd).wait_send()


def field_kernel(runs, chunk, maps_ref, incoming_ref, near_ref, out_ref):
    first = pl.program_id(0) * chunk
    samples = near_ref.shape[-1]
    held = incoming_ref[...]
    for i in range(chunk):
        total = jnp.dot(maps_ref[first + i], held, preferred_element_type=F32)
        for j in range(runs):
            part = total[:, j * samples : (j + 1) * samples]
            out_ref[j, i] = (part + near_ref[j, first + i].astype(F32)).astype(BF16)


def per_device(
    currents,
    leaf_parent,
    near_links,
    near_blocks,
    aggregate_maps,
    far_boxes,
    far_counts,
    translate_coef,
    time_kernel,
    disaggregate_maps,
):
    boxes, dirs = lax.axis_size("box"), lax.axis_size("dir")
    devices = boxes * dirs
    leaf_count, unknowns, samples = currents.shape
    leaf_top, directions, _ = aggregate_maps.shape
    runs = leaf_count // leaf_top
    top_local, list_slots = far_boxes.shape
    rows = directions // dirs
    plane = top_local * rows
    chunks = leaf_top // AGG_CHUNK
    width = -(-devices * runs // 128) * 128

    held = functools.partial(pltpu.with_memory_space_constraint, memory_space=pltpu.HBM)
    hbm = pl.BlockSpec(memory_space=pltpu.HBM)
    vmem = pl.BlockSpec(memory_space=pltpu.VMEM)
    smem = pl.BlockSpec(memory_space=pltpu.SMEM)
    dma = pltpu.SemaphoreType.DMA
    incoming, near, maps = pl.pallas_call(
        functools.partial(rays_kernel, boxes, dirs, runs),
        out_shape=(
            jax.ShapeDtypeStruct((directions, runs * samples), BF16),
            jax.ShapeDtypeStruct((runs, leaf_top, unknowns, samples), BF16),
            jax.ShapeDtypeStruct(disaggregate_maps.shape, BF16),
        ),
        in_specs=[hbm, hbm, hbm, hbm, vmem, smem, smem, vmem, smem, smem],
        out_specs=(vmem, vmem, vmem),
        scratch_shapes=[
            pltpu.VMEM((leaf_count + 2, unknowns, samples), BF16),
            pltpu.VMEM((directions, runs * samples), F32),
            pltpu.VMEM((runs, directions, samples), BF16),
            pltpu.VMEM((boxes, dirs, runs, rows, samples), BF16),
            pltpu.VMEM((1, width), F32),
            pltpu.VMEM((devices, 1, width), F32),
            pltpu.VMEM((top_local, list_slots, 128), F32),
            pltpu.VMEM((top_local, 128, width), F32),
            pltpu.VMEM((top_local, rows, width), F32),
            pltpu.VMEM((2 * plane, width), BF16),
            pltpu.VMEM((boxes, 2 * plane, plane), BF16),
            pltpu.VMEM((2 * plane, samples), F32),
            pltpu.VMEM((2 * samples, 2 * samples), BF16),
            pltpu.VMEM((dirs, rows, runs * samples), BF16),
            pltpu.VMEM((dirs, rows, runs * samples), BF16),
            dma((chunks,)),
            dma((runs, chunks)),
            dma,
            dma,
            dma((devices,)),
            dma((devices,)),
            dma((devices,)),
            dma((devices,)),
            dma((dirs,)),
            dma((dirs,)),
            dma((2,)),
            dma((2,)),
        ],
        compiler_params=pltpu.CompilerParams(
            collective_id=0, has_side_effects=True, vmem_limit_bytes=30 * 2**20
        ),
        name="rays",
    )(
        held(currents),
        held(aggregate_maps),
        held(disaggregate_maps),
        held(translate_coef),
        held(near_blocks),
        held(near_links.T),
        held(leaf_parent),
        held(far_boxes),
        held(far_counts),
        held(time_kernel),
    )

    chunk = 8
    out = pl.pallas_call(
        functools.partial(field_kernel, runs, chunk),
        out_shape=jax.ShapeDtypeStruct((runs, leaf_top, unknowns, samples), BF16),
        grid=(leaf_top // chunk,),
        in_specs=[vmem, vmem, vmem],
        out_specs=pl.BlockSpec((runs, chunk, unknowns, samples), lambda i: (0, i, 0, 0)),
        name="field",
        compiler_params=pltpu.CompilerParams(vmem_limit_bytes=6 * 2**20),
    )(maps, incoming, near)
    return out.reshape(leaf_count, unknowns, samples)


def solution(mesh):
    return jax.shard_map(
        per_device,
        mesh=mesh,
        in_specs=(
            P(("box", "dir"), None, None),
            P(("box", "dir")),
            P(("box", "dir"), None),
            P(),
            P(),
            P("box", None),
            P("box"),
            P("box", None, None),
            P(),
            P(),
        ),
        out_specs=P(("box", "dir"), None, None),
        check_vma=False,
    )
```

```python
import functools
import jax
import jax.numpy as jnp
from jax import lax
from jax.experimental import pallas as pl
from jax.experimental.pallas import tpu as pltpu
from jax.sharding import PartitionSpec as P

MESH = pl.DeviceIdType.MESH
F32 = jnp.float32
BF16 = jnp.bfloat16
AGG_CHUNK = 4
NEAR_BLOCK = 8
REACH = 2
RELAY_FROM = 2


def split_high_low(value):
    high = value.astype(BF16)
    return high, (value - high.astype(F32)).astype(BF16)


def rays_kernel(
    boxes,
    dirs,
    runs,
    cur_hbm,
    agg_hbm,
    dis_hbm,
    coef_hbm,
    blocks_hbm,
    links_hbm,
    leaf_parent_hbm,
    lists_hbm,
    counts_hbm,
    kernel_hbm,
    incoming_ref,
    near_ref,
    dis_ref,
    leaf,
    acc,
    rays,
    rays_all,
    blocks_ref,
    links_ref,
    leaf_parent_ref,
    lists_ref,
    counts_ref,
    kernel_ref,
    parent_row_ref,
    parent_all,
    coef,
    weights_ref,
    split_ref,
    spread_ref,
    far_ref,
    time_ref,
    stage_ref,
    landed,
    agg_sem,
    cur_sem,
    small_sem,
    dis_sem,
    par_send,
    par_recv,
    ray_send,
    ray_recv,
    relay_send,
    back_send,
    back_recv,
    rim_send,
    rim_recv,
):
    my_box = lax.axis_index("box")
    my_dir = lax.axis_index("dir")
    me = my_box * dirs + my_dir
    devices = boxes * dirs
    leaf_top = agg_hbm.shape[0]
    samples = cur_hbm.shape[-1]
    directions = agg_hbm.shape[1]
    rows = directions // dirs
    top_local = counts_ref.shape[0]
    slots = lists_ref.shape[1]
    width = parent_row_ref.shape[-1]
    places = dirs * runs
    group = far_ref.shape[1] // 2
    cut = group // places
    leaves = runs * leaf_top
    dot = functools.partial(jnp.dot, preferred_element_type=F32)
    peers = [(kb, kd) for kb in range(boxes) for kd in range(dirs) if kb or kd]

    def target(kb, kd):
        return lax.rem(my_box + kb, boxes), lax.rem(my_dir + kd, dirs)

    chunks = leaf_top // AGG_CHUNK

    def loads(c):
        first = c * AGG_CHUNK
        out = []
        for j in range(runs):
            at = j * leaf_top + first
            out.append(
                pltpu.make_async_copy(
                    cur_hbm.at[pl.ds(at, AGG_CHUNK)],
                    leaf.at[pl.ds(at + 1, AGG_CHUNK)],
                    cur_sem.at[j, c],
                )
            )
        out.append(
            pltpu.make_async_copy(
                agg_hbm.at[pl.ds(first, AGG_CHUNK)],
                dis_ref.at[pl.ds(first, AGG_CHUNK)],
                agg_sem.at[c],
            )
        )
        return out

    def start_loads(c, carry):
        for copy in loads(c):
            copy.start()
        return carry

    block_at = my_dir * rows
    lane_tile = lax.div(block_at, 128) * 128
    small = [
        (leaf_parent_hbm, leaf_parent_ref),
        (links_hbm, links_ref),
        (counts_hbm, counts_ref),
        (kernel_hbm, kernel_ref),
        (lists_hbm, lists_ref),
        (blocks_hbm, blocks_ref),
        (coef_hbm.at[:, :, pl.ds(pl.multiple_of(lane_tile, 128), 128)], coef),
    ]
    small = [pltpu.make_async_copy(a, b, small_sem.at[i]) for i, (a, b) in enumerate(small)]
    small[0].start()
    lax.fori_loop(0, chunks, start_loads, 0)
    for copy in small[1:]:
        copy.start()

    barrier = pltpu.get_barrier_semaphore()
    for kb, kd in peers:
        tb, td = target(kb, kd)
        pl.semaphore_signal(
            barrier, inc=1, device_id={"box": tb, "dir": td}, device_id_type=MESH
        )

    @pl.when(me == 0)
    def _():
        leaf[0] = jnp.zeros(leaf.shape[1:], BF16)

    @pl.when(me == devices - 1)
    def _():
        leaf[leaves + 1] = jnp.zeros(leaf.shape[1:], BF16)

    small[0].wait()
    lane = lax.broadcasted_iota(jnp.int32, (1, width), 1)
    spare = jnp.where(me == 0, -1, 0)
    parent_row = jnp.where(lane >= devices * runs, spare, jnp.zeros((1, width), jnp.int32))
    for j in range(runs):
        parent_row = jnp.where(lane == me * runs + j, leaf_parent_ref[j * leaf_top], parent_row)
    parent_row_ref[...] = parent_row.astype(F32)
    parent_all[me] = parent_row.astype(F32)
    acc[...] = jnp.zeros_like(acc)

    def aggregate(c, carry):
        for copy in loads(c):
            copy.wait()
        first = c * AGG_CHUNK
        maps = jnp.concatenate([dis_ref[first + i] for i in range(AGG_CHUNK)], axis=1)
        held = jnp.concatenate(
            [
                jnp.concatenate([leaf[1 + j * leaf_top + first + i] for j in range(runs)], axis=1)
                for i in range(AGG_CHUNK)
            ],
            axis=0,
        )
        acc[...] += dot(maps, held)
        return carry

    lax.fori_loop(0, chunks, aggregate, 0)

    def parent_copy(kb, kd):
        tb, td = target(kb, kd)
        return pltpu.make_async_remote_copy(
            src_ref=parent_row_ref,
            dst_ref=parent_all.at[me],
            send_sem=par_send.at[tb * dirs + td],
            recv_sem=par_recv.at[me],
            device_id={"box": tb, "dir": td},
            device_id_type=MESH,
        )

    def ray_copy(delta, kd):
        tb = my_box + delta
        td = lax.rem(my_dir + kd, dirs)
        block = pl.ds(pl.multiple_of(td * rows, rows), rows)
        return pltpu.make_async_remote_copy(
            src_ref=rays.at[:, block, :],
            dst_ref=rays_all.at[my_box, my_dir],
            send_sem=ray_send.at[(delta + REACH) * dirs + td],
            recv_sem=ray_recv.at[me],
            device_id={"box": tb, "dir": td},
            device_id_type=MESH,
        )

    def relay_copy(side, away, sd):
        sb = my_box - side * away
        slot = sb * dirs + sd
        return pltpu.make_async_remote_copy(
            src_ref=rays_all.at[sb, sd],
            dst_ref=rays_all.at[sb, sd],
            send_sem=relay_send.at[slot],
            recv_sem=ray_recv.at[slot],
            device_id={"box": my_box + side, "dir": my_dir},
            device_id_type=MESH,
        )

    def rim_copy(side):
        other = lax.rem(me + (1 if side == 0 else devices - 1), devices)
        return pltpu.make_async_remote_copy(
            src_ref=cur_hbm.at[leaves - 1 if side == 0 else 0],
            dst_ref=leaf.at[0 if side == 0 else leaves + 1],
            send_sem=rim_send.at[side],
            recv_sem=rim_recv.at[side],
            device_id={"box": lax.div(other, dirs), "dir": lax.rem(other, dirs)},
            device_id_type=MESH,
        )

    def inside(box):
        return jnp.logical_and(box >= 0, box < boxes)

    def when_sending(delta, action):
        def every():
            for kd in range(dirs):
                if delta or kd:
                    action(ray_copy(delta, kd))

        if delta:
            pl.when(inside(my_box + delta))(every)
        else:
            every()

    for j in range(runs):
        rays[j] = acc[:, j * samples : (j + 1) * samples].astype(BF16)
    pl.semaphore_wait(barrier, len(peers))
    deltas = sorted(range(-REACH, REACH + 1), key=lambda delta: -abs(delta))
    deltas = [delta for delta in deltas if abs(delta) < boxes]
    for delta in deltas:
        when_sending(delta, lambda copy: copy.start())
    for kb, kd in peers:
        parent_copy(kb, kd).start()

    @pl.when(me < devices - 1)
    def _():
        rim_copy(0).start()

    @pl.when(me > 0)
    def _():
        rim_copy(1).start()

    own = pl.ds(pl.multiple_of(block_at, rows), rows)
    rays_all[my_box, my_dir] = rays[:, own, :]
    dis_copy = pltpu.make_async_copy(dis_hbm, dis_ref, dis_sem)
    dis_copy.start()
    for copy in small[1:]:
        copy.wait()

    def near_block(step):
        first = step * NEAR_BLOCK
        pairs = [
            jnp.concatenate([leaf[j * leaf_top + first + u] for j in range(runs)], axis=1)
            for u in range(NEAR_BLOCK + 2)
        ]
        for u in range(NEAR_BLOCK):
            mid = dot(blocks_ref[0], pairs[u + 1])
            low = dot(blocks_ref[1], pairs[u])
            high = dot(blocks_ref[2], pairs[u + 2])
            for j in range(runs):
                span = slice(j * samples, (j + 1) * samples)
                at = j * leaf_top + first + u
                with_low = links_ref[0, at].astype(F32)
                with_high = links_ref[1, at].astype(F32)
                part = mid[:, span] + with_low * low[:, span] + with_high * high[:, span]
                near_ref[j, first + u] = part.astype(BF16)

    def arrived(ref, send_sem, recv_sem):
        pltpu.make_async_remote_copy(
            src_ref=ref,
            dst_ref=ref,
            send_sem=send_sem,
            recv_sem=recv_sem,
            device_id={"box": my_box, "dir": lax.rem(my_dir + 1, dirs)},
            device_id_type=MESH,
        ).wait_recv()

    def ray_arrived(sb, sd):
        slot = sb * dirs + sd
        arrived(rays_all.at[sb, sd], relay_send.at[slot], ray_recv.at[slot])

    def each_relay(action):
        for away in range(REACH, boxes - 1):
            for side in (1, -1):
                fits = jnp.logical_and(inside(my_box - side * away), inside(my_box + side))
                pl.when(fits)(functools.partial(action, side, away))

    blocks = leaf_top // NEAR_BLOCK
    per_step = -(-dirs // (blocks - 2 - RELAY_FROM))

    def near_step(step, carry):
        near_block(step + 1)

        @pl.when(step >= RELAY_FROM)
        def _():
            def forward(side, away):
                for i in range(per_step):
                    sd = (step - RELAY_FROM) * per_step + i

                    @pl.when(sd < dirs)
                    def _():
                        ray_arrived(my_box - side * away, sd)
                        relay_copy(side, away, sd).start()

            each_relay(forward)

        return carry

    lax.fori_loop(0, blocks - 2, near_step, 0)

    spread_time = pltpu.roll(
        jnp.broadcast_to(kernel_ref[...], (samples, samples)), 0, 1, stride=1, stride_axis=0
    )
    causal = lax.broadcasted_iota(jnp.int32, (samples, samples), 1) >= lax.broadcasted_iota(
        jnp.int32, (samples, samples), 0
    )
    time_high, time_low = split_high_low(jnp.where(causal, spread_time, 0.0))
    time_ref[:samples, :samples] = time_high
    time_ref[:samples, samples:] = time_low
    time_ref[samples:, :samples] = time_high
    time_ref[samples:, samples:] = jnp.zeros_like(time_low)

    for kb, kd in peers:
        sb, sd = target(kb, kd)
        slot = sb * dirs + sd
        arrived(parent_all.at[slot], par_send.at[slot], par_recv.at[slot])
    parents = jnp.zeros((1, width), F32)
    for slot in range(devices):
        parents = parents + parent_all[slot]
    column = jnp.broadcast_to(parents, (128, width)).T[:, :slots]
    spot = lax.broadcasted_iota(jnp.int32, (1, slots), 1)
    turn = lax.rem(128 - (block_at - lane_tile), 128)
    for c in range(top_local):
        used = jnp.where(spot < counts_ref[c], lists_ref[c : c + 1, :], -2)
        match = (column == used.astype(F32)).astype(F32).astype(BF16)
        high, low = split_high_low(pltpu.roll(coef[c], turn, 1)[:, :rows])
        both = lax.dot_general(
            jnp.concatenate([high, low], axis=1),
            match,
            (((0,), (1,)), ((), ())),
            preferred_element_type=F32,
        )
        high, low = split_high_low(both[:rows, :] + both[rows:, :])
        weights_ref[c * rows : (c + 1) * rows, :width] = high
        weights_ref[c * rows : (c + 1) * rows, width:] = low

    def iota(shape, axis):
        return lax.broadcasted_iota(jnp.int32, shape, axis)

    total = places * rows
    for g in range(total // group):
        place = lax.div(iota((group, width), 0), cut)
        here = iota((group, width), 1) == my_box * places + place
        parent = jnp.sum(jnp.where(here, parents, 0.0), axis=1, keepdims=True)
        shape = (group, total)
        owner = (my_box * top_local + lax.div(iota(shape, 1), rows)).astype(F32)
        same = lax.rem(iota(shape, 1), rows) == g * cut + lax.rem(iota(shape, 0), cut)
        pick = jnp.where(jnp.logical_and(parent == owner, same), 1.0, 0.0).astype(BF16)
        moved = dot(pick, weights_ref[...]).astype(BF16)
        split_ref[g, :group, :] = moved[:, :width]
        split_ref[g, group:, :] = moved[:, width:]

    def spread(b, carry):
        shape = (width, group)
        pick = iota(shape, 0) == b * places + lax.div(iota(shape, 1), cut)
        pick = jnp.where(pick, 1.0, 0.0).astype(BF16)
        shape = (2 * group, group)
        same = lax.rem(iota(shape, 0), cut) == lax.rem(iota(shape, 1), cut)
        for g in range(total // group):
            spread_ref[b, g] = jnp.where(same, dot(split_ref[g], pick), 0.0).astype(BF16)
        return carry

    lax.fori_loop(0, boxes, spread, 0)

    half = lax.div(my_box * 2, boxes)
    for n in range(boxes):
        sb = lax.rem(my_box + n * (1 - 2 * half) + boxes, boxes)

        def plain():
            for kd in range(1 if n == 0 else 0, dirs):
                ray_arrived(sb, lax.rem(my_dir + kd, dirs))

        if n == 0:
            plain()
        else:
            up = jnp.logical_and(sb <= my_box - REACH, my_box + 1 < boxes)
            down = jnp.logical_and(sb >= my_box + REACH, my_box >= 1)
            pl.when(jnp.logical_not(jnp.logical_or(up, down)))(plain)
        for g in range(total // group):
            held = rays_all[sb, :, :, g * cut : (g + 1) * cut, :].reshape(group, samples)
            part_sum = dot(spread_ref[sb, g], held)
            if n == 0:
                far_ref[g] = part_sum
            else:
                far_ref[g] += part_sum

    for g in range(total // group):
        high, low = split_high_low(far_ref[g, :group, :] + far_ref[g, group:, :])
        both = dot(jnp.concatenate([high, low], axis=1), time_ref[...])
        incoming = (both[:, :samples] + both[:, samples:]).astype(BF16)
        for d in range(dirs):
            for j in range(runs):
                place = d * runs + j
                stage_ref[d, g * cut : (g + 1) * cut, j * samples : (j + 1) * samples] = incoming[
                    place * cut : (place + 1) * cut, :
                ]

    def back_copy(kd):
        td = lax.rem(my_dir + kd, dirs)
        return pltpu.make_async_remote_copy(
            src_ref=stage_ref.at[td],
            dst_ref=landed.at[my_dir],
            send_sem=back_send.at[td],
            recv_sem=back_recv.at[my_dir],
            device_id={"box": my_box, "dir": td},
            device_id_type=MESH,
        )

    for kd in range(1, dirs):
        back_copy(kd).start()
    landed[my_dir] = stage_ref[my_dir]

    @pl.when(me < devices - 1)
    def _():
        rim_copy(0).wait_send()
        rim_copy(1).wait_recv()

    @pl.when(me > 0)
    def _():
        rim_copy(1).wait_send()
        rim_copy(0).wait_recv()

    def last_block(step, carry):
        near_block(step * (blocks - 1))
        return carry

    lax.fori_loop(0, 2, last_block, 0)
    for kb, kd in peers:
        parent_copy(kb, kd).wait_send()
    for delta in deltas:
        when_sending(delta, lambda copy: copy.wait_send())

    def relayed(side, away):
        for sd in range(dirs):
            relay_copy(side, away, sd).wait_send()

    each_relay(relayed)
    dis_copy.wait()
    for kd in range(1, dirs):
        sd = lax.rem(my_dir + kd, dirs)
        arrived(landed.at[sd], back_send.at[sd], back_recv.at[sd])
    incoming_ref[...] = landed[...].reshape(directions, runs * samples)
    for kd in range(1, dirs):
        back_copy(kd).wait_send()


def field_kernel(runs, chunk, maps_ref, incoming_ref, near_ref, out_ref, held_out, sem):
    leaf_top, _, _ = maps_ref.shape
    samples = near_ref.shape[-1]
    held = incoming_ref[...]

    def copy(step):
        span = pl.ds(step * chunk, chunk)
        return pltpu.make_async_copy(held_out.at[:, span], out_ref.at[:, span], sem.at[step])

    def step_of(step, carry):
        for i in range(chunk):
            at = step * chunk + i
            total = jnp.dot(maps_ref[at], held, preferred_element_type=F32)
            for j in range(runs):
                part = total[:, j * samples : (j + 1) * samples]
                held_out[j, at] = (part + near_ref[j, at].astype(F32)).astype(BF16)
        copy(step).start()
        return carry

    def finish(step, carry):
        copy(step).wait()
        return carry

    steps = leaf_top // chunk
    lax.fori_loop(0, steps, step_of, 0, unroll=4)
    lax.fori_loop(0, steps, finish, 0)


def per_device(
    currents,
    leaf_parent,
    near_links,
    near_blocks,
    aggregate_maps,
    far_boxes,
    far_counts,
    translate_coef,
    time_kernel,
    disaggregate_maps,
):
    boxes, dirs = lax.axis_size("box"), lax.axis_size("dir")
    devices = boxes * dirs
    leaf_count, unknowns, samples = currents.shape
    leaf_top, directions, _ = aggregate_maps.shape
    runs = leaf_count // leaf_top
    top_local, list_slots = far_boxes.shape
    rows = directions // dirs
    plane = top_local * rows
    cut = min(rows, 16)
    group = top_local * cut
    groups = rows // cut
    chunks = leaf_top // AGG_CHUNK
    width = -(-devices * runs // 128) * 128

    held = functools.partial(pltpu.with_memory_space_constraint, memory_space=pltpu.HBM)
    hbm = pl.BlockSpec(memory_space=pltpu.HBM)
    vmem = pl.BlockSpec(memory_space=pltpu.VMEM)
    smem = pl.BlockSpec(memory_space=pltpu.SMEM)
    dma = pltpu.SemaphoreType.DMA
    incoming, near, maps = pl.pallas_call(
        functools.partial(rays_kernel, boxes, dirs, runs),
        out_shape=(
            jax.ShapeDtypeStruct((directions, runs * samples), BF16),
            jax.ShapeDtypeStruct((runs, leaf_top, unknowns, samples), BF16),
            jax.ShapeDtypeStruct(disaggregate_maps.shape, BF16),
        ),
        in_specs=[hbm] * 10,
        out_specs=(vmem, vmem, vmem),
        scratch_shapes=[
            pltpu.VMEM((leaf_count + 2, unknowns, samples), BF16),
            pltpu.VMEM((directions, runs * samples), F32),
            pltpu.VMEM((runs, directions, samples), BF16),
            pltpu.VMEM((boxes, dirs, runs, rows, samples), BF16),
            pltpu.VMEM(near_blocks.shape, BF16),
            pltpu.SMEM((2, leaf_count), jnp.int32),
            pltpu.SMEM((leaf_count,), jnp.int32),
            pltpu.VMEM((top_local, list_slots), jnp.int32),
            pltpu.SMEM((top_local,), jnp.int32),
            pltpu.VMEM((1, samples), F32),
            pltpu.VMEM((1, width), F32),
            pltpu.VMEM((devices, 1, width), F32),
            pltpu.VMEM((top_local, list_slots, 128), F32),
            pltpu.VMEM((plane, 2 * width), BF16),
            pltpu.VMEM((groups, 2 * group, width), BF16),
            pltpu.VMEM((boxes, groups, 2 * group, group), BF16),
            pltpu.VMEM((groups, 2 * group, samples), F32),
            pltpu.VMEM((2 * samples, 2 * samples), BF16),
            pltpu.VMEM((dirs, rows, runs * samples), BF16),
            pltpu.VMEM((dirs, rows, runs * samples), BF16),
            dma((chunks,)),
            dma((runs, chunks)),
            dma((7,)),
            dma,
            dma((devices,)),
            dma((devices,)),
            dma(((2 * REACH + 1) * dirs,)),
            dma((devices,)),
            dma((devices,)),
            dma((dirs,)),
            dma((dirs,)),
            dma((2,)),
            dma((2,)),
        ],
        compiler_params=pltpu.CompilerParams(
            collective_id=0, has_side_effects=True, vmem_limit_bytes=30 * 2**20
        ),
        name="rays",
    )(
        held(currents),
        held(aggregate_maps),
        held(disaggregate_maps),
        held(translate_coef),
        held(near_blocks),
        held(near_links.T),
        held(leaf_parent),
        held(far_boxes),
        held(far_counts),
        held(time_kernel.reshape(1, samples)),
    )

    chunk = 4
    out_shape = (runs, leaf_top, unknowns, samples)
    out = pl.pallas_call(
        functools.partial(field_kernel, runs, chunk),
        out_shape=jax.ShapeDtypeStruct(out_shape, BF16),
        in_specs=[vmem, vmem, vmem],
        out_specs=hbm,
        scratch_shapes=[pltpu.VMEM(out_shape, BF16), dma((leaf_top // chunk,))],
        name="field",
        compiler_params=pltpu.CompilerParams(vmem_limit_bytes=10 * 2**20),
    )(maps, incoming, near)
    return out.reshape(leaf_count, unknowns, samples)


def solution(mesh):
    return jax.shard_map(
        per_device,
        mesh=mesh,
        in_specs=(
            P(("box", "dir"), None, None),
            P(("box", "dir")),
            P(("box", "dir"), None),
            P(),
            P(),
            P("box", None),
            P("box"),
            P("box", None, None),
            P(),
            P(),
        ),
        out_specs=P(("box", "dir"), None, None),
        check_vma=False,
    )
```

```python
import functools
import jax
import jax.numpy as jnp
from jax import lax
from jax.experimental import pallas as pl
from jax.experimental.pallas import tpu as pltpu
from jax.sharding import PartitionSpec as P

MESH = pl.DeviceIdType.MESH
F32 = jnp.float32
BF16 = jnp.bfloat16
AGG_CHUNK = 4
NEAR_BLOCK = 8
REACH = 2
EARLY_BLOCKS = 3


def split_high_low(value):
    high = value.astype(BF16)
    return high, (value - high.astype(F32)).astype(BF16)


def rays_kernel(
    boxes,
    dirs,
    runs,
    cur_hbm,
    agg_hbm,
    dis_hbm,
    coef_hbm,
    blocks_hbm,
    links_hbm,
    leaf_parent_hbm,
    lists_hbm,
    counts_hbm,
    kernel_hbm,
    incoming_ref,
    near_ref,
    dis_ref,
    leaf,
    acc,
    rays,
    rays_all,
    blocks_ref,
    links_ref,
    leaf_parent_ref,
    lists_ref,
    counts_ref,
    kernel_ref,
    parent_row_ref,
    parent_all,
    coef,
    weights_ref,
    split_ref,
    spread_ref,
    far_ref,
    time_ref,
    stage_ref,
    landed,
    agg_sem,
    cur_sem,
    small_sem,
    dis_sem,
    par_send,
    par_recv,
    ray_send,
    ray_recv,
    relay_send,
    back_send,
    back_recv,
    rim_send,
    rim_recv,
):
    my_box = lax.axis_index("box")
    my_dir = lax.axis_index("dir")
    me = my_box * dirs + my_dir
    devices = boxes * dirs
    leaf_top = agg_hbm.shape[0]
    samples = cur_hbm.shape[-1]
    directions = agg_hbm.shape[1]
    rows = directions // dirs
    top_local = counts_ref.shape[0]
    slots = lists_ref.shape[1]
    width = parent_row_ref.shape[-1]
    places = dirs * runs
    group = far_ref.shape[1] // 2
    cut = group // places
    leaves = runs * leaf_top
    dot = functools.partial(jnp.dot, preferred_element_type=F32)
    peers = [(kb, kd) for kb in range(boxes) for kd in range(dirs) if kb or kd]

    def target(kb, kd):
        return lax.rem(my_box + kb, boxes), lax.rem(my_dir + kd, dirs)

    chunks = leaf_top // AGG_CHUNK

    def loads(c):
        first = c * AGG_CHUNK
        out = []
        for j in range(runs):
            at = j * leaf_top + first
            out.append(
                pltpu.make_async_copy(
                    cur_hbm.at[pl.ds(at, AGG_CHUNK)],
                    leaf.at[pl.ds(at + 1, AGG_CHUNK)],
                    cur_sem.at[j, c],
                )
            )
        out.append(
            pltpu.make_async_copy(
                agg_hbm.at[pl.ds(first, AGG_CHUNK)],
                dis_ref.at[pl.ds(first, AGG_CHUNK)],
                agg_sem.at[c],
            )
        )
        return out

    def start_loads(c, carry):
        for copy in loads(c):
            copy.start()
        return carry

    block_at = my_dir * rows
    lane_tile = lax.div(block_at, 128) * 128
    small = [
        (leaf_parent_hbm, leaf_parent_ref),
        (links_hbm, links_ref),
        (counts_hbm, counts_ref),
        (kernel_hbm, kernel_ref),
        (lists_hbm, lists_ref),
        (blocks_hbm, blocks_ref),
        (coef_hbm.at[:, :, pl.ds(pl.multiple_of(lane_tile, 128), 128)], coef),
    ]
    small = [pltpu.make_async_copy(a, b, small_sem.at[i]) for i, (a, b) in enumerate(small)]
    small[0].start()
    lax.fori_loop(0, chunks, start_loads, 0)

    barrier = pltpu.get_barrier_semaphore()
    for kb, kd in peers:
        tb, td = target(kb, kd)
        pl.semaphore_signal(
            barrier, inc=1, device_id={"box": tb, "dir": td}, device_id_type=MESH
        )

    @pl.when(me == 0)
    def _():
        leaf[0] = jnp.zeros(leaf.shape[1:], BF16)

    @pl.when(me == devices - 1)
    def _():
        leaf[leaves + 1] = jnp.zeros(leaf.shape[1:], BF16)

    small[0].wait()
    lane = lax.broadcasted_iota(jnp.int32, (1, width), 1)
    spare = jnp.where(me == 0, -1, 0)
    parent_row = jnp.where(lane >= devices * runs, spare, jnp.zeros((1, width), jnp.int32))
    for j in range(runs):
        parent_row = jnp.where(lane == me * runs + j, leaf_parent_ref[j * leaf_top], parent_row)
    parent_row_ref[...] = parent_row.astype(F32)
    parent_all[me] = parent_row.astype(F32)
    acc[...] = jnp.zeros_like(acc)

    def aggregate(c, carry):
        for copy in loads(c):
            copy.wait()
        first = c * AGG_CHUNK
        maps = jnp.concatenate([dis_ref[first + i] for i in range(AGG_CHUNK)], axis=1)
        held = jnp.concatenate(
            [
                jnp.concatenate([leaf[1 + j * leaf_top + first + i] for j in range(runs)], axis=1)
                for i in range(AGG_CHUNK)
            ],
            axis=0,
        )
        acc[...] += dot(maps, held)
        return carry

    lax.fori_loop(0, chunks - 2, aggregate, 0)
    for copy in small[1:]:
        copy.start()
    lax.fori_loop(chunks - 2, chunks, aggregate, 0)

    def parent_copy(kb, kd):
        tb, td = target(kb, kd)
        return pltpu.make_async_remote_copy(
            src_ref=parent_row_ref,
            dst_ref=parent_all.at[me],
            send_sem=par_send.at[tb * dirs + td],
            recv_sem=par_recv.at[me],
            device_id={"box": tb, "dir": td},
            device_id_type=MESH,
        )

    def ray_copy(delta, kd):
        tb = my_box + delta
        td = lax.rem(my_dir + kd, dirs)
        block = pl.ds(pl.multiple_of(td * rows, rows), rows)
        return pltpu.make_async_remote_copy(
            src_ref=rays.at[:, block, :],
            dst_ref=rays_all.at[my_box, my_dir],
            send_sem=ray_send.at[(delta + REACH) * dirs + td],
            recv_sem=ray_recv.at[me],
            device_id={"box": tb, "dir": td},
            device_id_type=MESH,
        )

    def relay_copy(side, away, sd):
        sb = my_box - side * away
        slot = sb * dirs + sd
        return pltpu.make_async_remote_copy(
            src_ref=rays_all.at[sb, sd],
            dst_ref=rays_all.at[sb, sd],
            send_sem=relay_send.at[slot],
            recv_sem=ray_recv.at[slot],
            device_id={"box": my_box + side, "dir": my_dir},
            device_id_type=MESH,
        )

    def rim_copy(side):
        other = lax.rem(me + (1 if side == 0 else devices - 1), devices)
        return pltpu.make_async_remote_copy(
            src_ref=cur_hbm.at[leaves - 1 if side == 0 else 0],
            dst_ref=leaf.at[0 if side == 0 else leaves + 1],
            send_sem=rim_send.at[side],
            recv_sem=rim_recv.at[side],
            device_id={"box": lax.div(other, dirs), "dir": lax.rem(other, dirs)},
            device_id_type=MESH,
        )

    def inside(box):
        return jnp.logical_and(box >= 0, box < boxes)

    def when_sending(delta, action):
        def every():
            for kd in range(dirs):
                if delta or kd:
                    action(ray_copy(delta, kd))

        if delta:
            pl.when(inside(my_box + delta))(every)
        else:
            every()

    for j in range(runs):
        rays[j] = acc[:, j * samples : (j + 1) * samples].astype(BF16)
    pl.semaphore_wait(barrier, len(peers))
    deltas = sorted(range(-REACH, REACH + 1), key=lambda delta: -abs(delta))
    deltas = [delta for delta in deltas if abs(delta) < boxes]
    for kb, kd in peers:
        parent_copy(kb, kd).start()
    for delta in deltas:
        when_sending(delta, lambda copy: copy.start())

    @pl.when(me < devices - 1)
    def _():
        rim_copy(0).start()

    @pl.when(me > 0)
    def _():
        rim_copy(1).start()

    own = pl.ds(pl.multiple_of(block_at, rows), rows)
    rays_all[my_box, my_dir] = rays[:, own, :]
    dis_copy = pltpu.make_async_copy(dis_hbm, dis_ref, dis_sem)
    dis_copy.start()
    for copy in small[1:]:
        copy.wait()

    def near_block(step):
        first = step * NEAR_BLOCK
        pairs = [
            jnp.concatenate([leaf[j * leaf_top + first + u] for j in range(runs)], axis=1)
            for u in range(NEAR_BLOCK + 2)
        ]
        for u in range(NEAR_BLOCK):
            mid = dot(blocks_ref[0], pairs[u + 1])
            low = dot(blocks_ref[1], pairs[u])
            high = dot(blocks_ref[2], pairs[u + 2])
            for j in range(runs):
                span = slice(j * samples, (j + 1) * samples)
                at = j * leaf_top + first + u
                with_low = links_ref[0, at].astype(F32)
                with_high = links_ref[1, at].astype(F32)
                part = mid[:, span] + with_low * low[:, span] + with_high * high[:, span]
                near_ref[j, first + u] = part.astype(BF16)

    def arrived(ref, send_sem, recv_sem):
        pltpu.make_async_remote_copy(
            src_ref=ref,
            dst_ref=ref,
            send_sem=send_sem,
            recv_sem=recv_sem,
            device_id={"box": my_box, "dir": lax.rem(my_dir + 1, dirs)},
            device_id_type=MESH,
        ).wait_recv()

    def ray_arrived(sb, sd):
        slot = sb * dirs + sd
        arrived(rays_all.at[sb, sd], relay_send.at[slot], ray_recv.at[slot])

    def each_relay(action):
        for away in range(REACH, boxes - 1):
            for side in (1, -1):
                fits = jnp.logical_and(inside(my_box - side * away), inside(my_box + side))
                pl.when(fits)(functools.partial(action, side, away))

    blocks = leaf_top // NEAR_BLOCK
    late_blocks = blocks - 2 - EARLY_BLOCKS
    per_step = dirs // (late_blocks + 1)

    def near_only(step, carry):
        near_block(step)
        return carry

    def relay(side, away, i, carry):
        sd = lax.rem(my_dir - i + dirs, dirs)
        ray_arrived(my_box - side * away, sd)
        relay_copy(side, away, sd).start()
        return carry

    def relay_span(first, last):
        def some(side, away):
            lax.fori_loop(first, last, functools.partial(relay, side, away), 0)

        each_relay(some)

    def near_relay(step, carry):
        near_block(step)
        first = (step - EARLY_BLOCKS - 1) * per_step
        relay_span(first, first + per_step)
        return carry

    lax.fori_loop(1, 1 + EARLY_BLOCKS, near_only, 0)
    lax.fori_loop(1 + EARLY_BLOCKS, blocks - 1, near_relay, 0)
    relay_span(late_blocks * per_step, dirs)

    spread_time = pltpu.roll(
        jnp.broadcast_to(kernel_ref[...], (samples, samples)), 0, 1, stride=1, stride_axis=0
    )
    causal = lax.broadcasted_iota(jnp.int32, (samples, samples), 1) >= lax.broadcasted_iota(
        jnp.int32, (samples, samples), 0
    )
    time_high, time_low = split_high_low(jnp.where(causal, spread_time, 0.0))
    time_ref[:samples, :samples] = time_high
    time_ref[:samples, samples:] = time_low
    time_ref[samples:, :samples] = time_high
    time_ref[samples:, samples:] = jnp.zeros_like(time_low)

    for kb, kd in peers:
        sb, sd = target(kb, kd)
        slot = sb * dirs + sd
        arrived(parent_all.at[slot], par_send.at[slot], par_recv.at[slot])
    parents = jnp.zeros((1, width), F32)
    for slot in range(devices):
        parents = parents + parent_all[slot]
    column = jnp.broadcast_to(parents, (128, width)).T[:, :slots]
    spot = lax.broadcasted_iota(jnp.int32, (1, slots), 1)
    turn = lax.rem(128 - (block_at - lane_tile), 128)
    for c in range(top_local):
        used = jnp.where(spot < counts_ref[c], lists_ref[c : c + 1, :], -2)
        match = (column == used.astype(F32)).astype(F32).astype(BF16)
        high, low = split_high_low(pltpu.roll(coef[c], turn, 1)[:, :rows])
        both = lax.dot_general(
            jnp.concatenate([high, low], axis=1),
            match,
            (((0,), (1,)), ((), ())),
            preferred_element_type=F32,
        )
        high, low = split_high_low(both[:rows, :] + both[rows:, :])
        weights_ref[c * rows : (c + 1) * rows, :width] = high
        weights_ref[c * rows : (c + 1) * rows, width:] = low

    def iota(shape, axis):
        return lax.broadcasted_iota(jnp.int32, shape, axis)

    total = places * rows
    for g in range(total // group):
        place = lax.div(iota((group, width), 0), cut)
        here = iota((group, width), 1) == my_box * places + place
        parent = jnp.sum(jnp.where(here, parents, 0.0), axis=1, keepdims=True)
        shape = (group, total)
        owner = (my_box * top_local + lax.div(iota(shape, 1), rows)).astype(F32)
        same = lax.rem(iota(shape, 1), rows) == g * cut + lax.rem(iota(shape, 0), cut)
        pick = jnp.where(jnp.logical_and(parent == owner, same), 1.0, 0.0).astype(BF16)
        moved = dot(pick, weights_ref[...]).astype(BF16)
        split_ref[g, :group, :] = moved[:, :width]
        split_ref[g, group:, :] = moved[:, width:]

    def spread(b, carry):
        shape = (width, group)
        pick = iota(shape, 0) == b * places + lax.div(iota(shape, 1), cut)
        pick = jnp.where(pick, 1.0, 0.0).astype(BF16)
        shape = (2 * group, group)
        same = lax.rem(iota(shape, 0), cut) == lax.rem(iota(shape, 1), cut)
        for g in range(total // group):
            spread_ref[b, g] = jnp.where(same, dot(split_ref[g], pick), 0.0).astype(BF16)
        return carry

    lax.fori_loop(0, boxes, spread, 0)
    half = lax.div(my_box * 2, boxes)
    for n in range(boxes):
        sb = lax.rem(my_box + n * (1 - 2 * half) + boxes, boxes)

        def plain():
            for kd in range(1 if n == 0 else 0, dirs):
                ray_arrived(sb, lax.rem(my_dir + kd, dirs))

        if n == 0:
            plain()
        else:
            up = jnp.logical_and(sb <= my_box - REACH, my_box + 1 < boxes)
            down = jnp.logical_and(sb >= my_box + REACH, my_box >= 1)
            pl.when(jnp.logical_not(jnp.logical_or(up, down)))(plain)
        for g in range(total // group):
            held = rays_all[sb, :, :, g * cut : (g + 1) * cut, :].reshape(group, samples)
            part_sum = dot(spread_ref[sb, g], held)
            if n == 0:
                far_ref[g] = part_sum
            else:
                far_ref[g] += part_sum

    for g in range(total // group):
        high, low = split_high_low(far_ref[g, :group, :] + far_ref[g, group:, :])
        both = dot(jnp.concatenate([high, low], axis=1), time_ref[...])
        incoming = (both[:, :samples] + both[:, samples:]).astype(BF16)
        for d in range(dirs):
            for j in range(runs):
                place = d * runs + j
                stage_ref[d, g * cut : (g + 1) * cut, j * samples : (j + 1) * samples] = incoming[
                    place * cut : (place + 1) * cut, :
                ]

    def back_copy(kd):
        td = lax.rem(my_dir + kd, dirs)
        return pltpu.make_async_remote_copy(
            src_ref=stage_ref.at[td],
            dst_ref=landed.at[my_dir],
            send_sem=back_send.at[td],
            recv_sem=back_recv.at[my_dir],
            device_id={"box": my_box, "dir": td},
            device_id_type=MESH,
        )

    for kd in range(1, dirs):
        back_copy(kd).start()
    landed[my_dir] = stage_ref[my_dir]

    @pl.when(me < devices - 1)
    def _():
        rim_copy(0).wait_send()
        rim_copy(1).wait_recv()

    @pl.when(me > 0)
    def _():
        rim_copy(1).wait_send()
        rim_copy(0).wait_recv()

    def last_block(step, carry):
        near_block(step * (blocks - 1))
        return carry

    lax.fori_loop(0, 2, last_block, 0)
    for kb, kd in peers:
        parent_copy(kb, kd).wait_send()
    for delta in deltas:
        when_sending(delta, lambda copy: copy.wait_send())

    def relayed(side, away):
        for sd in range(dirs):
            relay_copy(side, away, sd).wait_send()

    each_relay(relayed)
    dis_copy.wait()
    for kd in range(1, dirs):
        sd = lax.rem(my_dir + kd, dirs)
        arrived(landed.at[sd], back_send.at[sd], back_recv.at[sd])
    incoming_ref[...] = landed[...].reshape(directions, runs * samples)
    for kd in range(1, dirs):
        back_copy(kd).wait_send()


def field_kernel(runs, chunk, maps_ref, incoming_ref, near_ref, out_ref, held_out, sem):
    leaf_top, _, _ = maps_ref.shape
    samples = near_ref.shape[-1]
    held = incoming_ref[...]

    def copy(step):
        span = pl.ds(step * chunk, chunk)
        return pltpu.make_async_copy(held_out.at[:, span], out_ref.at[:, span], sem.at[step])

    def step_of(step, carry):
        for i in range(chunk):
            at = step * chunk + i
            total = jnp.dot(maps_ref[at], held, preferred_element_type=F32)
            for j in range(runs):
                part = total[:, j * samples : (j + 1) * samples]
                held_out[j, at] = (part + near_ref[j, at].astype(F32)).astype(BF16)
        copy(step).start()
        return carry

    def finish(step, carry):
        copy(step).wait()
        return carry

    steps = leaf_top // chunk
    lax.fori_loop(0, steps, step_of, 0, unroll=4)
    lax.fori_loop(0, steps, finish, 0)


def per_device(
    currents,
    leaf_parent,
    near_links,
    near_blocks,
    aggregate_maps,
    far_boxes,
    far_counts,
    translate_coef,
    time_kernel,
    disaggregate_maps,
):
    boxes, dirs = lax.axis_size("box"), lax.axis_size("dir")
    devices = boxes * dirs
    leaf_count, unknowns, samples = currents.shape
    leaf_top, directions, _ = aggregate_maps.shape
    runs = leaf_count // leaf_top
    top_local, list_slots = far_boxes.shape
    rows = directions // dirs
    plane = top_local * rows
    cut = min(rows, 16)
    group = top_local * cut
    groups = rows // cut
    chunks = leaf_top // AGG_CHUNK
    width = -(-devices * runs // 128) * 128

    held = functools.partial(pltpu.with_memory_space_constraint, memory_space=pltpu.HBM)
    hbm = pl.BlockSpec(memory_space=pltpu.HBM)
    vmem = pl.BlockSpec(memory_space=pltpu.VMEM)
    smem = pl.BlockSpec(memory_space=pltpu.SMEM)
    dma = pltpu.SemaphoreType.DMA
    incoming, near, maps = pl.pallas_call(
        functools.partial(rays_kernel, boxes, dirs, runs),
        out_shape=(
            jax.ShapeDtypeStruct((directions, runs * samples), BF16),
            jax.ShapeDtypeStruct((runs, leaf_top, unknowns, samples), BF16),
            jax.ShapeDtypeStruct(disaggregate_maps.shape, BF16),
        ),
        in_specs=[hbm] * 10,
        out_specs=(vmem, vmem, vmem),
        scratch_shapes=[
            pltpu.VMEM((leaf_count + 2, unknowns, samples), BF16),
            pltpu.VMEM((directions, runs * samples), F32),
            pltpu.VMEM((runs, directions, samples), BF16),
            pltpu.VMEM((boxes, dirs, runs, rows, samples), BF16),
            pltpu.VMEM(near_blocks.shape, BF16),
            pltpu.SMEM((2, leaf_count), jnp.int32),
            pltpu.SMEM((leaf_count,), jnp.int32),
            pltpu.VMEM((top_local, list_slots), jnp.int32),
            pltpu.SMEM((top_local,), jnp.int32),
            pltpu.VMEM((1, samples), F32),
            pltpu.VMEM((1, width), F32),
            pltpu.VMEM((devices, 1, width), F32),
            pltpu.VMEM((top_local, list_slots, 128), F32),
            pltpu.VMEM((plane, 2 * width), BF16),
            pltpu.VMEM((groups, 2 * group, width), BF16),
            pltpu.VMEM((boxes, groups, 2 * group, group), BF16),
            pltpu.VMEM((groups, 2 * group, samples), F32),
            pltpu.VMEM((2 * samples, 2 * samples), BF16),
            pltpu.VMEM((dirs, rows, runs * samples), BF16),
            pltpu.VMEM((dirs, rows, runs * samples), BF16),
            dma((chunks,)),
            dma((runs, chunks)),
            dma((7,)),
            dma,
            dma((devices,)),
            dma((devices,)),
            dma(((2 * REACH + 1) * dirs,)),
            dma((devices,)),
            dma((devices,)),
            dma((dirs,)),
            dma((dirs,)),
            dma((2,)),
            dma((2,)),
        ],
        compiler_params=pltpu.CompilerParams(
            collective_id=0, has_side_effects=True, vmem_limit_bytes=30 * 2**20
        ),
        name="rays",
    )(
        held(currents),
        held(aggregate_maps),
        held(disaggregate_maps),
        held(translate_coef),
        held(near_blocks),
        held(near_links.T),
        held(leaf_parent),
        held(far_boxes),
        held(far_counts),
        held(time_kernel.reshape(1, samples)),
    )

    chunk = 4
    out_shape = (runs, leaf_top, unknowns, samples)
    out = pl.pallas_call(
        functools.partial(field_kernel, runs, chunk),
        out_shape=jax.ShapeDtypeStruct(out_shape, BF16),
        in_specs=[vmem, vmem, vmem],
        out_specs=hbm,
        scratch_shapes=[pltpu.VMEM(out_shape, BF16), dma((leaf_top // chunk,))],
        name="field",
        compiler_params=pltpu.CompilerParams(vmem_limit_bytes=10 * 2**20),
    )(maps, incoming, near)
    return out.reshape(leaf_count, unknowns, samples)


def solution(mesh):
    return jax.shard_map(
        per_device,
        mesh=mesh,
        in_specs=(
            P(("box", "dir"), None, None),
            P(("box", "dir")),
            P(("box", "dir"), None),
            P(),
            P(),
            P("box", None),
            P("box"),
            P("box", None, None),
            P(),
            P(),
        ),
        out_specs=P(("box", "dir"), None, None),
        check_vma=False,
    )
```

```python
import functools
import jax
import jax.numpy as jnp
from jax import lax
from jax.experimental import pallas as pl
from jax.experimental.pallas import tpu as pltpu
from jax.sharding import PartitionSpec as P

MESH = pl.DeviceIdType.MESH
F32 = jnp.float32
BF16 = jnp.bfloat16
AGG_CHUNK = 4
NEAR_BLOCK = 8
REACH = 2
EARLY_BLOCKS = 3


def split_high_low(value):
    high = value.astype(BF16)
    return high, (value - high.astype(F32)).astype(BF16)


def rays_kernel(
    boxes,
    dirs,
    runs,
    cur_hbm,
    agg_hbm,
    dis_hbm,
    coef_hbm,
    blocks_hbm,
    links_hbm,
    leaf_parent_hbm,
    lists_hbm,
    counts_hbm,
    kernel_hbm,
    incoming_ref,
    near_ref,
    dis_ref,
    leaf,
    acc,
    rays,
    rays_all,
    blocks_ref,
    links_ref,
    leaf_parent_ref,
    lists_ref,
    counts_ref,
    kernel_ref,
    parent_row_ref,
    parent_all,
    coef,
    weights_ref,
    split_ref,
    spread_ref,
    far_ref,
    time_ref,
    stage_ref,
    landed,
    agg_sem,
    cur_sem,
    small_sem,
    dis_sem,
    par_send,
    par_recv,
    ray_send,
    ray_recv,
    relay_send,
    back_send,
    back_recv,
    rim_send,
    rim_recv,
):
    my_box = lax.axis_index("box")
    my_dir = lax.axis_index("dir")
    me = my_box * dirs + my_dir
    devices = boxes * dirs
    leaf_top = agg_hbm.shape[0]
    samples = cur_hbm.shape[-1]
    directions = agg_hbm.shape[1]
    rows = directions // dirs
    top_local = counts_ref.shape[0]
    slots = lists_ref.shape[1]
    width = parent_row_ref.shape[-1]
    places = dirs * runs
    group = far_ref.shape[1] // 2
    cut = group // places
    leaves = runs * leaf_top
    dot = functools.partial(jnp.dot, preferred_element_type=F32)
    peers = [(kb, kd) for kb in range(boxes) for kd in range(dirs) if kb or kd]

    def target(kb, kd):
        return lax.rem(my_box + kb, boxes), lax.rem(my_dir + kd, dirs)

    chunks = leaf_top // AGG_CHUNK

    def loads(c):
        first = c * AGG_CHUNK
        out = []
        for j in range(runs):
            at = j * leaf_top + first
            out.append(
                pltpu.make_async_copy(
                    cur_hbm.at[pl.ds(at, AGG_CHUNK)],
                    leaf.at[pl.ds(at + 1, AGG_CHUNK)],
                    cur_sem.at[j, c],
                )
            )
        out.append(
            pltpu.make_async_copy(
                agg_hbm.at[pl.ds(first, AGG_CHUNK)],
                dis_ref.at[pl.ds(first, AGG_CHUNK)],
                agg_sem.at[c],
            )
        )
        return out

    def start_loads(c, carry):
        for copy in loads(c):
            copy.start()
        return carry

    block_at = my_dir * rows
    lane_tile = lax.div(block_at, 128) * 128
    small = [
        (leaf_parent_hbm, leaf_parent_ref),
        (links_hbm, links_ref),
        (counts_hbm, counts_ref),
        (kernel_hbm, kernel_ref),
        (lists_hbm, lists_ref),
        (blocks_hbm, blocks_ref),
        (coef_hbm.at[:, :, pl.ds(pl.multiple_of(lane_tile, 128), 128)], coef),
    ]
    small = [pltpu.make_async_copy(a, b, small_sem.at[i]) for i, (a, b) in enumerate(small)]
    small[0].start()
    lax.fori_loop(0, chunks, start_loads, 0)

    barrier = pltpu.get_barrier_semaphore()
    for kb, kd in peers:
        tb, td = target(kb, kd)
        pl.semaphore_signal(
            barrier, inc=1, device_id={"box": tb, "dir": td}, device_id_type=MESH
        )

    @pl.when(me == 0)
    def _():
        leaf[0] = jnp.zeros(leaf.shape[1:], BF16)

    @pl.when(me == devices - 1)
    def _():
        leaf[leaves + 1] = jnp.zeros(leaf.shape[1:], BF16)

    small[0].wait()
    lane = lax.broadcasted_iota(jnp.int32, (1, width), 1)
    spare = jnp.where(me == 0, -1, 0)
    parent_row = jnp.where(lane >= devices * runs, spare, jnp.zeros((1, width), jnp.int32))
    for j in range(runs):
        parent_row = jnp.where(lane == me * runs + j, leaf_parent_ref[j * leaf_top], parent_row)
    parent_row_ref[...] = parent_row.astype(F32)
    parent_all[me] = parent_row.astype(F32)
    acc[...] = jnp.zeros_like(acc)

    def aggregate(c, carry):
        for copy in loads(c):
            copy.wait()
        first = c * AGG_CHUNK
        maps = jnp.concatenate([dis_ref[first + i] for i in range(AGG_CHUNK)], axis=1)
        held = jnp.concatenate(
            [
                jnp.concatenate([leaf[1 + j * leaf_top + first + i] for j in range(runs)], axis=1)
                for i in range(AGG_CHUNK)
            ],
            axis=0,
        )
        acc[...] += dot(maps, held)
        return carry

    def parent_copy(kb, kd):
        tb, td = target(kb, kd)
        return pltpu.make_async_remote_copy(
            src_ref=parent_row_ref,
            dst_ref=parent_all.at[me],
            send_sem=par_send.at[tb * dirs + td],
            recv_sem=par_recv.at[me],
            device_id={"box": tb, "dir": td},
            device_id_type=MESH,
        )

    lax.fori_loop(0, chunks - 4, aggregate, 0)
    for copy in small[1:]:
        copy.start()
    pl.semaphore_wait(barrier, len(peers))
    for kb, kd in peers:
        parent_copy(kb, kd).start()
    lax.fori_loop(chunks - 4, chunks, aggregate, 0)

    def ray_copy(delta, kd):
        tb = my_box + delta
        td = lax.rem(my_dir + kd, dirs)
        block = pl.ds(pl.multiple_of(td * rows, rows), rows)
        return pltpu.make_async_remote_copy(
            src_ref=rays.at[:, block, :],
            dst_ref=rays_all.at[my_box, my_dir],
            send_sem=ray_send.at[(delta + REACH) * dirs + td],
            recv_sem=ray_recv.at[me],
            device_id={"box": tb, "dir": td},
            device_id_type=MESH,
        )

    def relay_copy(side, away, sd):
        sb = my_box - side * away
        slot = sb * dirs + sd
        return pltpu.make_async_remote_copy(
            src_ref=rays_all.at[sb, sd],
            dst_ref=rays_all.at[sb, sd],
            send_sem=relay_send.at[slot],
            recv_sem=ray_recv.at[slot],
            device_id={"box": my_box + side, "dir": my_dir},
            device_id_type=MESH,
        )

    def rim_copy(side):
        other = lax.rem(me + (1 if side == 0 else devices - 1), devices)
        return pltpu.make_async_remote_copy(
            src_ref=cur_hbm.at[leaves - 1 if side == 0 else 0],
            dst_ref=leaf.at[0 if side == 0 else leaves + 1],
            send_sem=rim_send.at[side],
            recv_sem=rim_recv.at[side],
            device_id={"box": lax.div(other, dirs), "dir": lax.rem(other, dirs)},
            device_id_type=MESH,
        )

    def inside(box):
        return jnp.logical_and(box >= 0, box < boxes)

    def when_sending(delta, action):
        def every():
            for kd in range(dirs):
                if delta or kd:
                    action(ray_copy(delta, kd))

        if delta:
            pl.when(inside(my_box + delta))(every)
        else:
            every()

    for j in range(runs):
        rays[j] = acc[:, j * samples : (j + 1) * samples].astype(BF16)
    deltas = sorted(range(-REACH, REACH + 1), key=lambda delta: -abs(delta))
    deltas = [delta for delta in deltas if abs(delta) < boxes]
    for delta in deltas:
        when_sending(delta, lambda copy: copy.start())

    @pl.when(me < devices - 1)
    def _():
        rim_copy(0).start()

    @pl.when(me > 0)
    def _():
        rim_copy(1).start()

    own = pl.ds(pl.multiple_of(block_at, rows), rows)
    rays_all[my_box, my_dir] = rays[:, own, :]
    dis_copy = pltpu.make_async_copy(dis_hbm, dis_ref, dis_sem)
    dis_copy.start()
    for copy in small[1:]:
        copy.wait()

    def near_block(step):
        first = step * NEAR_BLOCK
        pairs = [
            jnp.concatenate([leaf[j * leaf_top + first + u] for j in range(runs)], axis=1)
            for u in range(NEAR_BLOCK + 2)
        ]
        for u in range(NEAR_BLOCK):
            mid = dot(blocks_ref[0], pairs[u + 1])
            low = dot(blocks_ref[1], pairs[u])
            high = dot(blocks_ref[2], pairs[u + 2])
            for j in range(runs):
                span = slice(j * samples, (j + 1) * samples)
                at = j * leaf_top + first + u
                with_low = links_ref[0, at].astype(F32)
                with_high = links_ref[1, at].astype(F32)
                part = mid[:, span] + with_low * low[:, span] + with_high * high[:, span]
                near_ref[j, first + u] = part.astype(BF16)

    def arrived(ref, send_sem, recv_sem):
        pltpu.make_async_remote_copy(
            src_ref=ref,
            dst_ref=ref,
            send_sem=send_sem,
            recv_sem=recv_sem,
            device_id={"box": my_box, "dir": lax.rem(my_dir + 1, dirs)},
            device_id_type=MESH,
        ).wait_recv()

    def ray_arrived(sb, sd):
        slot = sb * dirs + sd
        arrived(rays_all.at[sb, sd], relay_send.at[slot], ray_recv.at[slot])

    def each_relay(action):
        for away in range(REACH, boxes - 1):
            for side in (1, -1):
                fits = jnp.logical_and(inside(my_box - side * away), inside(my_box + side))
                pl.when(fits)(functools.partial(action, side, away))

    blocks = leaf_top // NEAR_BLOCK
    late_blocks = blocks - 2 - EARLY_BLOCKS
    per_step = dirs // (late_blocks + 1)

    def near_only(step, carry):
        near_block(step)
        return carry

    def relay(side, away, i, carry):
        sd = lax.rem(my_dir - i + dirs, dirs)
        ray_arrived(my_box - side * away, sd)
        relay_copy(side, away, sd).start()
        return carry

    def relay_span(first, last):
        def some(side, away):
            lax.fori_loop(first, last, functools.partial(relay, side, away), 0)

        each_relay(some)

    def near_relay(step, carry):
        near_block(step)
        first = (step - EARLY_BLOCKS - 1) * per_step
        relay_span(first, first + per_step)
        return carry

    lax.fori_loop(1, 1 + EARLY_BLOCKS, near_only, 0)
    lax.fori_loop(1 + EARLY_BLOCKS, blocks - 1, near_relay, 0)
    relay_span(late_blocks * per_step, dirs)

    spread_time = pltpu.roll(
        jnp.broadcast_to(kernel_ref[...], (samples, samples)), 0, 1, stride=1, stride_axis=0
    )
    causal = lax.broadcasted_iota(jnp.int32, (samples, samples), 1) >= lax.broadcasted_iota(
        jnp.int32, (samples, samples), 0
    )
    time_high, time_low = split_high_low(jnp.where(causal, spread_time, 0.0))
    time_ref[:samples, :samples] = time_high
    time_ref[:samples, samples:] = time_low
    time_ref[samples:, :samples] = time_high
    time_ref[samples:, samples:] = jnp.zeros_like(time_low)

    for kb, kd in peers:
        sb, sd = target(kb, kd)
        slot = sb * dirs + sd
        arrived(parent_all.at[slot], par_send.at[slot], par_recv.at[slot])
    parents = jnp.zeros((1, width), F32)
    for slot in range(devices):
        parents = parents + parent_all[slot]
    column = jnp.broadcast_to(parents, (128, width)).T[:, :slots]
    spot = lax.broadcasted_iota(jnp.int32, (1, slots), 1)
    turn = lax.rem(128 - (block_at - lane_tile), 128)
    for c in range(top_local):
        used = jnp.where(spot < counts_ref[c], lists_ref[c : c + 1, :], -2)
        match = (column == used.astype(F32)).astype(F32).astype(BF16)
        high, low = split_high_low(pltpu.roll(coef[c], turn, 1)[:, :rows])
        both = lax.dot_general(
            jnp.concatenate([high, low], axis=1),
            match,
            (((0,), (1,)), ((), ())),
            preferred_element_type=F32,
        )
        high, low = split_high_low(both[:rows, :] + both[rows:, :])
        weights_ref[c * rows : (c + 1) * rows, :width] = high
        weights_ref[c * rows : (c + 1) * rows, width:] = low

    def iota(shape, axis):
        return lax.broadcasted_iota(jnp.int32, shape, axis)

    total = places * rows
    for g in range(total // group):
        place = lax.div(iota((group, width), 0), cut)
        here = iota((group, width), 1) == my_box * places + place
        parent = jnp.sum(jnp.where(here, parents, 0.0), axis=1, keepdims=True)
        shape = (group, total)
        owner = (my_box * top_local + lax.div(iota(shape, 1), rows)).astype(F32)
        same = lax.rem(iota(shape, 1), rows) == g * cut + lax.rem(iota(shape, 0), cut)
        pick = jnp.where(jnp.logical_and(parent == owner, same), 1.0, 0.0).astype(BF16)
        moved = dot(pick, weights_ref[...]).astype(BF16)
        split_ref[g, :group, :] = moved[:, :width]
        split_ref[g, group:, :] = moved[:, width:]

    def spread(b, carry):
        shape = (width, group)
        pick = iota(shape, 0) == b * places + lax.div(iota(shape, 1), cut)
        pick = jnp.where(pick, 1.0, 0.0).astype(BF16)
        shape = (2 * group, group)
        same = lax.rem(iota(shape, 0), cut) == lax.rem(iota(shape, 1), cut)
        for g in range(total // group):
            spread_ref[b, g] = jnp.where(same, dot(split_ref[g], pick), 0.0).astype(BF16)
        return carry

    lax.fori_loop(0, boxes, spread, 0)
    half = lax.div(my_box * 2, boxes)
    for n in range(boxes):
        sb = lax.rem(my_box + n * (1 - 2 * half) + boxes, boxes)

        def plain():
            for kd in range(1 if n == 0 else 0, dirs):
                ray_arrived(sb, lax.rem(my_dir + kd, dirs))

        if n == 0:
            plain()
        else:
            up = jnp.logical_and(sb <= my_box - REACH, my_box + 1 < boxes)
            down = jnp.logical_and(sb >= my_box + REACH, my_box >= 1)
            pl.when(jnp.logical_not(jnp.logical_or(up, down)))(plain)
        for g in range(total // group):
            held = rays_all[sb, :, :, g * cut : (g + 1) * cut, :].reshape(group, samples)
            part_sum = dot(spread_ref[sb, g], held)
            if n == 0:
                far_ref[g] = part_sum
            else:
                far_ref[g] += part_sum

    for g in range(total // group):
        high, low = split_high_low(far_ref[g, :group, :] + far_ref[g, group:, :])
        both = dot(jnp.concatenate([high, low], axis=1), time_ref[...])
        incoming = (both[:, :samples] + both[:, samples:]).astype(BF16)
        for d in range(dirs):
            for j in range(runs):
                place = d * runs + j
                stage_ref[d, g * cut : (g + 1) * cut, j * samples : (j + 1) * samples] = incoming[
                    place * cut : (place + 1) * cut, :
                ]

    def back_copy(kd):
        td = lax.rem(my_dir + kd, dirs)
        return pltpu.make_async_remote_copy(
            src_ref=stage_ref.at[td],
            dst_ref=landed.at[my_dir],
            send_sem=back_send.at[td],
            recv_sem=back_recv.at[my_dir],
            device_id={"box": my_box, "dir": td},
            device_id_type=MESH,
        )

    for kd in range(1, dirs):
        back_copy(kd).start()
    landed[my_dir] = stage_ref[my_dir]

    @pl.when(me < devices - 1)
    def _():
        rim_copy(0).wait_send()
        rim_copy(1).wait_recv()

    @pl.when(me > 0)
    def _():
        rim_copy(1).wait_send()
        rim_copy(0).wait_recv()

    def last_block(step, carry):
        near_block(step * (blocks - 1))
        return carry

    lax.fori_loop(0, 2, last_block, 0)
    for kb, kd in peers:
        parent_copy(kb, kd).wait_send()
    for delta in deltas:
        when_sending(delta, lambda copy: copy.wait_send())

    def relayed(side, away):
        for sd in range(dirs):
            relay_copy(side, away, sd).wait_send()

    each_relay(relayed)
    dis_copy.wait()
    for kd in range(1, dirs):
        sd = lax.rem(my_dir + kd, dirs)
        arrived(landed.at[sd], back_send.at[sd], back_recv.at[sd])
    incoming_ref[...] = landed[...].reshape(directions, runs * samples)
    for kd in range(1, dirs):
        back_copy(kd).wait_send()


def field_kernel(runs, chunk, maps_ref, incoming_ref, near_ref, out_ref, held_out, sem):
    leaf_top, _, _ = maps_ref.shape
    samples = near_ref.shape[-1]
    held = incoming_ref[...]

    def copy(step):
        span = pl.ds(step * chunk, chunk)
        return pltpu.make_async_copy(held_out.at[:, span], out_ref.at[:, span], sem.at[step])

    def step_of(step, carry):
        for i in range(chunk):
            at = step * chunk + i
            total = jnp.dot(maps_ref[at], held, preferred_element_type=F32)
            for j in range(runs):
                part = total[:, j * samples : (j + 1) * samples]
                held_out[j, at] = (part + near_ref[j, at].astype(F32)).astype(BF16)
        copy(step).start()
        return carry

    def finish(step, carry):
        copy(step).wait()
        return carry

    steps = leaf_top // chunk
    lax.fori_loop(0, steps, step_of, 0, unroll=8)
    lax.fori_loop(0, steps, finish, 0)


def per_device(
    currents,
    leaf_parent,
    near_links,
    near_blocks,
    aggregate_maps,
    far_boxes,
    far_counts,
    translate_coef,
    time_kernel,
    disaggregate_maps,
):
    boxes, dirs = lax.axis_size("box"), lax.axis_size("dir")
    devices = boxes * dirs
    leaf_count, unknowns, samples = currents.shape
    leaf_top, directions, _ = aggregate_maps.shape
    runs = leaf_count // leaf_top
    top_local, list_slots = far_boxes.shape
    rows = directions // dirs
    plane = top_local * rows
    cut = min(rows, 16)
    group = top_local * cut
    groups = rows // cut
    chunks = leaf_top // AGG_CHUNK
    width = -(-devices * runs // 128) * 128

    held = functools.partial(pltpu.with_memory_space_constraint, memory_space=pltpu.HBM)
    hbm = pl.BlockSpec(memory_space=pltpu.HBM)
    vmem = pl.BlockSpec(memory_space=pltpu.VMEM)
    smem = pl.BlockSpec(memory_space=pltpu.SMEM)
    dma = pltpu.SemaphoreType.DMA
    incoming, near, maps = pl.pallas_call(
        functools.partial(rays_kernel, boxes, dirs, runs),
        out_shape=(
            jax.ShapeDtypeStruct((directions, runs * samples), BF16),
            jax.ShapeDtypeStruct((runs, leaf_top, unknowns, samples), BF16),
            jax.ShapeDtypeStruct(disaggregate_maps.shape, BF16),
        ),
        in_specs=[hbm] * 10,
        out_specs=(vmem, vmem, vmem),
        scratch_shapes=[
            pltpu.VMEM((leaf_count + 2, unknowns, samples), BF16),
            pltpu.VMEM((directions, runs * samples), F32),
            pltpu.VMEM((runs, directions, samples), BF16),
            pltpu.VMEM((boxes, dirs, runs, rows, samples), BF16),
            pltpu.VMEM(near_blocks.shape, BF16),
            pltpu.SMEM((2, leaf_count), jnp.int32),
            pltpu.SMEM((leaf_count,), jnp.int32),
            pltpu.VMEM((top_local, list_slots), jnp.int32),
            pltpu.SMEM((top_local,), jnp.int32),
            pltpu.VMEM((1, samples), F32),
            pltpu.VMEM((1, width), F32),
            pltpu.VMEM((devices, 1, width), F32),
            pltpu.VMEM((top_local, list_slots, 128), F32),
            pltpu.VMEM((plane, 2 * width), BF16),
            pltpu.VMEM((groups, 2 * group, width), BF16),
            pltpu.VMEM((boxes, groups, 2 * group, group), BF16),
            pltpu.VMEM((groups, 2 * group, samples), F32),
            pltpu.VMEM((2 * samples, 2 * samples), BF16),
            pltpu.VMEM((dirs, rows, runs * samples), BF16),
            pltpu.VMEM((dirs, rows, runs * samples), BF16),
            dma((chunks,)),
            dma((runs, chunks)),
            dma((7,)),
            dma,
            dma((devices,)),
            dma((devices,)),
            dma(((2 * REACH + 1) * dirs,)),
            dma((devices,)),
            dma((devices,)),
            dma((dirs,)),
            dma((dirs,)),
            dma((2,)),
            dma((2,)),
        ],
        compiler_params=pltpu.CompilerParams(
            collective_id=0, has_side_effects=True, vmem_limit_bytes=30 * 2**20
        ),
        name="rays",
    )(
        held(currents),
        held(aggregate_maps),
        held(disaggregate_maps),
        held(translate_coef),
        held(near_blocks),
        held(near_links.T),
        held(leaf_parent),
        held(far_boxes),
        held(far_counts),
        held(time_kernel.reshape(1, samples)),
    )

    chunk = 4
    out_shape = (runs, leaf_top, unknowns, samples)
    out = pl.pallas_call(
        functools.partial(field_kernel, runs, chunk),
        out_shape=jax.ShapeDtypeStruct(out_shape, BF16),
        in_specs=[vmem, vmem, vmem],
        out_specs=hbm,
        scratch_shapes=[pltpu.VMEM(out_shape, BF16), dma((leaf_top // chunk,))],
        name="field",
        compiler_params=pltpu.CompilerParams(vmem_limit_bytes=10 * 2**20),
    )(maps, incoming, near)
    return out.reshape(leaf_count, unknowns, samples)


def solution(mesh):
    return jax.shard_map(
        per_device,
        mesh=mesh,
        in_specs=(
            P(("box", "dir"), None, None),
            P(("box", "dir")),
            P(("box", "dir"), None),
            P(),
            P(),
            P("box", None),
            P("box"),
            P("box", None, None),
            P(),
            P(),
        ),
        out_specs=P(("box", "dir"), None, None),
        check_vma=False,
    )
```

```python
import functools
import jax
import jax.numpy as jnp
from jax import lax
from jax.experimental import pallas as pl
from jax.experimental.pallas import tpu as pltpu
from jax.sharding import PartitionSpec as P

MESH = pl.DeviceIdType.MESH
F32 = jnp.float32
BF16 = jnp.bfloat16
AGG_CHUNK = 4
NEAR_BLOCK = 8
REACH = 2
EARLY_BLOCKS = 3


def split_high_low(value):
    high = value.astype(BF16)
    return high, (value - high.astype(F32)).astype(BF16)


def rays_kernel(
    boxes,
    dirs,
    runs,
    cur_hbm,
    agg_hbm,
    dis_hbm,
    coef_hbm,
    blocks_hbm,
    links_hbm,
    leaf_parent_hbm,
    lists_hbm,
    counts_hbm,
    kernel_hbm,
    incoming_ref,
    near_ref,
    dis_ref,
    leaf,
    acc,
    rays,
    rays_all,
    blocks_ref,
    links_ref,
    leaf_parent_ref,
    lists_ref,
    counts_ref,
    kernel_ref,
    parent_row_ref,
    parent_all,
    coef,
    weights_ref,
    split_ref,
    spread_ref,
    far_ref,
    time_ref,
    stage_ref,
    landed,
    agg_sem,
    cur_sem,
    small_sem,
    dis_sem,
    par_send,
    par_recv,
    ray_send,
    ray_recv,
    relay_send,
    back_send,
    back_recv,
    rim_send,
    rim_recv,
):
    my_box = lax.axis_index("box")
    my_dir = lax.axis_index("dir")
    me = my_box * dirs + my_dir
    devices = boxes * dirs
    leaf_top = agg_hbm.shape[0]
    samples = cur_hbm.shape[-1]
    directions = agg_hbm.shape[1]
    rows = directions // dirs
    top_local = counts_ref.shape[0]
    slots = lists_ref.shape[1]
    width = parent_row_ref.shape[-1]
    places = dirs * runs
    group = far_ref.shape[1] // 2
    cut = group // places
    leaves = runs * leaf_top
    dot = functools.partial(jnp.dot, preferred_element_type=F32)
    peers = [(kb, kd) for kb in range(boxes) for kd in range(dirs) if kb or kd]

    def target(kb, kd):
        return lax.rem(my_box + kb, boxes), lax.rem(my_dir + kd, dirs)

    chunks = leaf_top // AGG_CHUNK

    def loads(c):
        first = c * AGG_CHUNK
        out = []
        for j in range(runs):
            at = j * leaf_top + first
            out.append(
                pltpu.make_async_copy(
                    cur_hbm.at[pl.ds(at, AGG_CHUNK)],
                    leaf.at[pl.ds(at + 1, AGG_CHUNK)],
                    cur_sem.at[j, c],
                )
            )
        out.append(
            pltpu.make_async_copy(
                agg_hbm.at[pl.ds(first, AGG_CHUNK)],
                dis_ref.at[pl.ds(first, AGG_CHUNK)],
                agg_sem.at[c],
            )
        )
        return out

    def start_loads(c, carry):
        for copy in loads(c):
            copy.start()
        return carry

    block_at = my_dir * rows
    lane_tile = lax.div(block_at, 128) * 128
    small = [
        (leaf_parent_hbm, leaf_parent_ref),
        (links_hbm, links_ref),
        (counts_hbm, counts_ref),
        (kernel_hbm, kernel_ref),
        (lists_hbm, lists_ref),
        (blocks_hbm, blocks_ref),
        (coef_hbm.at[:, :, pl.ds(pl.multiple_of(lane_tile, 128), 128)], coef),
    ]
    small = [pltpu.make_async_copy(a, b, small_sem.at[i]) for i, (a, b) in enumerate(small)]
    small[0].start()
    lax.fori_loop(0, chunks, start_loads, 0)

    barrier = pltpu.get_barrier_semaphore()
    for kb, kd in peers:
        tb, td = target(kb, kd)
        pl.semaphore_signal(
            barrier, inc=1, device_id={"box": tb, "dir": td}, device_id_type=MESH
        )

    @pl.when(me == 0)
    def _():
        leaf[0] = jnp.zeros(leaf.shape[1:], BF16)

    @pl.when(me == devices - 1)
    def _():
        leaf[leaves + 1] = jnp.zeros(leaf.shape[1:], BF16)

    small[0].wait()
    lane = lax.broadcasted_iota(jnp.int32, (1, width), 1)
    spare = jnp.where(me == 0, -1, 0)
    parent_row = jnp.where(lane >= devices * runs, spare, jnp.zeros((1, width), jnp.int32))
    for j in range(runs):
        parent_row = jnp.where(lane == me * runs + j, leaf_parent_ref[j * leaf_top], parent_row)
    parent_row_ref[...] = parent_row.astype(F32)
    parent_all[me] = parent_row.astype(F32)
    acc[...] = jnp.zeros_like(acc)

    def aggregate(c, carry):
        for copy in loads(c):
            copy.wait()
        first = c * AGG_CHUNK
        maps = jnp.concatenate([dis_ref[first + i] for i in range(AGG_CHUNK)], axis=1)
        held = jnp.concatenate(
            [
                jnp.concatenate([leaf[1 + j * leaf_top + first + i] for j in range(runs)], axis=1)
                for i in range(AGG_CHUNK)
            ],
            axis=0,
        )
        acc[...] += dot(maps, held)
        return carry

    def parent_copy(kb, kd):
        tb, td = target(kb, kd)
        return pltpu.make_async_remote_copy(
            src_ref=parent_row_ref,
            dst_ref=parent_all.at[me],
            send_sem=par_send.at[tb * dirs + td],
            recv_sem=par_recv.at[me],
            device_id={"box": tb, "dir": td},
            device_id_type=MESH,
        )

    lax.fori_loop(0, chunks - 6, aggregate, 0)
    for copy in small[1:]:
        copy.start()
    pl.semaphore_wait(barrier, len(peers))
    for kb, kd in peers:
        parent_copy(kb, kd).start()
    lax.fori_loop(chunks - 6, chunks, aggregate, 0)

    def ray_copy(delta, kd):
        tb = my_box + delta
        td = lax.rem(my_dir + kd, dirs)
        block = pl.ds(pl.multiple_of(td * rows, rows), rows)
        return pltpu.make_async_remote_copy(
            src_ref=rays.at[:, block, :],
            dst_ref=rays_all.at[my_box, my_dir],
            send_sem=ray_send.at[(delta + REACH) * dirs + td],
            recv_sem=ray_recv.at[me],
            device_id={"box": tb, "dir": td},
            device_id_type=MESH,
        )

    def relay_copy(side, away, sd):
        sb = my_box - side * away
        slot = sb * dirs + sd
        return pltpu.make_async_remote_copy(
            src_ref=rays_all.at[sb, sd],
            dst_ref=rays_all.at[sb, sd],
            send_sem=relay_send.at[slot],
            recv_sem=ray_recv.at[slot],
            device_id={"box": my_box + side, "dir": my_dir},
            device_id_type=MESH,
        )

    def rim_copy(side):
        other = lax.rem(me + (1 if side == 0 else devices - 1), devices)
        return pltpu.make_async_remote_copy(
            src_ref=cur_hbm.at[leaves - 1 if side == 0 else 0],
            dst_ref=leaf.at[0 if side == 0 else leaves + 1],
            send_sem=rim_send.at[side],
            recv_sem=rim_recv.at[side],
            device_id={"box": lax.div(other, dirs), "dir": lax.rem(other, dirs)},
            device_id_type=MESH,
        )

    def inside(box):
        return jnp.logical_and(box >= 0, box < boxes)

    def when_sending(delta, action):
        def every():
            for kd in range(dirs):
                if delta or kd:
                    action(ray_copy(delta, kd))

        if delta:
            pl.when(inside(my_box + delta))(every)
        else:
            every()

    for j in range(runs):
        rays[j] = acc[:, j * samples : (j + 1) * samples].astype(BF16)
    deltas = sorted(range(-REACH, REACH + 1), key=lambda delta: -abs(delta))
    deltas = [delta for delta in deltas if abs(delta) < boxes]
    for delta in deltas:
        when_sending(delta, lambda copy: copy.start())

    @pl.when(me < devices - 1)
    def _():
        rim_copy(0).start()

    @pl.when(me > 0)
    def _():
        rim_copy(1).start()

    own = pl.ds(pl.multiple_of(block_at, rows), rows)
    rays_all[my_box, my_dir] = rays[:, own, :]
    dis_copy = pltpu.make_async_copy(dis_hbm, dis_ref, dis_sem)
    dis_copy.start()
    for copy in small[1:]:
        copy.wait()

    def near_block(step):
        first = step * NEAR_BLOCK
        pairs = [
            jnp.concatenate([leaf[j * leaf_top + first + u] for j in range(runs)], axis=1)
            for u in range(NEAR_BLOCK + 2)
        ]
        for u in range(NEAR_BLOCK):
            mid = dot(blocks_ref[0], pairs[u + 1])
            low = dot(blocks_ref[1], pairs[u])
            high = dot(blocks_ref[2], pairs[u + 2])
            for j in range(runs):
                span = slice(j * samples, (j + 1) * samples)
                at = j * leaf_top + first + u
                with_low = links_ref[0, at].astype(F32)
                with_high = links_ref[1, at].astype(F32)
                part = mid[:, span] + with_low * low[:, span] + with_high * high[:, span]
                near_ref[j, first + u] = part.astype(BF16)

    def arrived(ref, send_sem, recv_sem):
        pltpu.make_async_remote_copy(
            src_ref=ref,
            dst_ref=ref,
            send_sem=send_sem,
            recv_sem=recv_sem,
            device_id={"box": my_box, "dir": lax.rem(my_dir + 1, dirs)},
            device_id_type=MESH,
        ).wait_recv()

    def ray_arrived(sb, sd):
        slot = sb * dirs + sd
        arrived(rays_all.at[sb, sd], relay_send.at[slot], ray_recv.at[slot])

    def each_relay(action):
        for away in range(REACH, boxes - 1):
            for side in (1, -1):
                fits = jnp.logical_and(inside(my_box - side * away), inside(my_box + side))
                pl.when(fits)(functools.partial(action, side, away))

    blocks = leaf_top // NEAR_BLOCK
    late_blocks = blocks - 2 - EARLY_BLOCKS
    per_step = dirs // (late_blocks + 1)

    def near_only(step, carry):
        near_block(step)
        return carry

    def relay(side, away, i, carry):
        sd = lax.rem(my_dir - i + dirs, dirs)
        ray_arrived(my_box - side * away, sd)
        relay_copy(side, away, sd).start()
        return carry

    def relay_span(first, last):
        def some(side, away):
            lax.fori_loop(first, last, functools.partial(relay, side, away), 0)

        each_relay(some)

    def near_relay(step, carry):
        near_block(step)
        first = (step - EARLY_BLOCKS - 1) * per_step
        relay_span(first, first + per_step)
        return carry

    lax.fori_loop(1, 1 + EARLY_BLOCKS, near_only, 0)
    lax.fori_loop(1 + EARLY_BLOCKS, blocks - 1, near_relay, 0)
    relay_span(late_blocks * per_step, dirs)

    spread_time = pltpu.roll(
        jnp.broadcast_to(kernel_ref[...], (samples, samples)), 0, 1, stride=1, stride_axis=0
    )
    causal = lax.broadcasted_iota(jnp.int32, (samples, samples), 1) >= lax.broadcasted_iota(
        jnp.int32, (samples, samples), 0
    )
    time_high, time_low = split_high_low(jnp.where(causal, spread_time, 0.0))
    time_ref[:samples, :samples] = time_high
    time_ref[:samples, samples:] = time_low
    time_ref[samples:, :samples] = time_high
    time_ref[samples:, samples:] = jnp.zeros_like(time_low)

    for kb, kd in peers:
        sb, sd = target(kb, kd)
        slot = sb * dirs + sd
        arrived(parent_all.at[slot], par_send.at[slot], par_recv.at[slot])
    parents = jnp.zeros((1, width), F32)
    for slot in range(devices):
        parents = parents + parent_all[slot]
    column = jnp.broadcast_to(parents, (128, width)).T[:, :slots]
    spot = lax.broadcasted_iota(jnp.int32, (1, slots), 1)
    turn = lax.rem(128 - (block_at - lane_tile), 128)
    for c in range(top_local):
        used = jnp.where(spot < counts_ref[c], lists_ref[c : c + 1, :], -2)
        match = (column == used.astype(F32)).astype(F32).astype(BF16)
        high, low = split_high_low(pltpu.roll(coef[c], turn, 1)[:, :rows])
        both = lax.dot_general(
            jnp.concatenate([high, low], axis=1),
            match,
            (((0,), (1,)), ((), ())),
            preferred_element_type=F32,
        )
        high, low = split_high_low(both[:rows, :] + both[rows:, :])
        weights_ref[c * rows : (c + 1) * rows, :width] = high
        weights_ref[c * rows : (c + 1) * rows, width:] = low

    def iota(shape, axis):
        return lax.broadcasted_iota(jnp.int32, shape, axis)

    total = places * rows
    for g in range(total // group):
        place = lax.div(iota((group, width), 0), cut)
        here = iota((group, width), 1) == my_box * places + place
        parent = jnp.sum(jnp.where(here, parents, 0.0), axis=1, keepdims=True)
        shape = (group, total)
        owner = (my_box * top_local + lax.div(iota(shape, 1), rows)).astype(F32)
        same = lax.rem(iota(shape, 1), rows) == g * cut + lax.rem(iota(shape, 0), cut)
        pick = jnp.where(jnp.logical_and(parent == owner, same), 1.0, 0.0).astype(BF16)
        moved = dot(pick, weights_ref[...]).astype(BF16)
        split_ref[g, :group, :] = moved[:, :width]
        split_ref[g, group:, :] = moved[:, width:]

    def spread(b, carry):
        shape = (width, group)
        pick = iota(shape, 0) == b * places + lax.div(iota(shape, 1), cut)
        pick = jnp.where(pick, 1.0, 0.0).astype(BF16)
        shape = (2 * group, group)
        same = lax.rem(iota(shape, 0), cut) == lax.rem(iota(shape, 1), cut)
        for g in range(total // group):
            spread_ref[b, g] = jnp.where(same, dot(split_ref[g], pick), 0.0).astype(BF16)
        return carry

    lax.fori_loop(0, boxes, spread, 0)
    half = lax.div(my_box * 2, boxes)
    for n in range(boxes):
        sb = lax.rem(my_box + n * (1 - 2 * half) + boxes, boxes)

        def plain():
            for kd in range(1 if n == 0 else 0, dirs):
                ray_arrived(sb, lax.rem(my_dir + kd, dirs))

        if n == 0:
            plain()
        else:
            up = jnp.logical_and(sb <= my_box - REACH, my_box + 1 < boxes)
            down = jnp.logical_and(sb >= my_box + REACH, my_box >= 1)
            pl.when(jnp.logical_not(jnp.logical_or(up, down)))(plain)
        for g in range(total // group):
            held = rays_all[sb, :, :, g * cut : (g + 1) * cut, :].reshape(group, samples)
            part_sum = dot(spread_ref[sb, g], held)
            if n == 0:
                far_ref[g] = part_sum
            else:
                far_ref[g] += part_sum

    for g in range(total // group):
        high, low = split_high_low(far_ref[g, :group, :] + far_ref[g, group:, :])
        both = dot(jnp.concatenate([high, low], axis=1), time_ref[...])
        incoming = (both[:, :samples] + both[:, samples:]).astype(BF16)
        for d in range(dirs):
            for j in range(runs):
                place = d * runs + j
                stage_ref[d, g * cut : (g + 1) * cut, j * samples : (j + 1) * samples] = incoming[
                    place * cut : (place + 1) * cut, :
                ]

    def back_copy(kd):
        td = lax.rem(my_dir + kd, dirs)
        return pltpu.make_async_remote_copy(
            src_ref=stage_ref.at[td],
            dst_ref=landed.at[my_dir],
            send_sem=back_send.at[td],
            recv_sem=back_recv.at[my_dir],
            device_id={"box": my_box, "dir": td},
            device_id_type=MESH,
        )

    for kd in range(1, dirs):
        back_copy(kd).start()
    landed[my_dir] = stage_ref[my_dir]

    @pl.when(me < devices - 1)
    def _():
        rim_copy(0).wait_send()
        rim_copy(1).wait_recv()

    @pl.when(me > 0)
    def _():
        rim_copy(1).wait_send()
        rim_copy(0).wait_recv()

    def last_block(step, carry):
        near_block(step * (blocks - 1))
        return carry

    lax.fori_loop(0, 2, last_block, 0)
    for kb, kd in peers:
        parent_copy(kb, kd).wait_send()
    for delta in deltas:
        when_sending(delta, lambda copy: copy.wait_send())

    def relayed(side, away):
        for sd in range(dirs):
            relay_copy(side, away, sd).wait_send()

    each_relay(relayed)
    dis_copy.wait()
    for kd in range(1, dirs):
        sd = lax.rem(my_dir + kd, dirs)
        arrived(landed.at[sd], back_send.at[sd], back_recv.at[sd])
    incoming_ref[...] = landed[...].reshape(directions, runs * samples)
    for kd in range(1, dirs):
        back_copy(kd).wait_send()


def field_kernel(runs, chunk, maps_ref, incoming_ref, near_ref, out_ref, held_out, sem):
    leaf_top, _, _ = maps_ref.shape
    samples = near_ref.shape[-1]
    held = incoming_ref[...]

    def copy(step):
        span = pl.ds(step * chunk, chunk)
        return pltpu.make_async_copy(held_out.at[:, span], out_ref.at[:, span], sem.at[step])

    def step_of(step, carry):
        for i in range(chunk):
            at = step * chunk + i
            total = jnp.dot(maps_ref[at], held, preferred_element_type=F32)
            for j in range(runs):
                part = total[:, j * samples : (j + 1) * samples]
                held_out[j, at] = (part + near_ref[j, at].astype(F32)).astype(BF16)
        copy(step).start()
        return carry

    def finish(step, carry):
        copy(step).wait()
        return carry

    steps = leaf_top // chunk
    lax.fori_loop(0, steps, step_of, 0, unroll=8)
    lax.fori_loop(0, steps, finish, 0)


def per_device(
    currents,
    leaf_parent,
    near_links,
    near_blocks,
    aggregate_maps,
    far_boxes,
    far_counts,
    translate_coef,
    time_kernel,
    disaggregate_maps,
):
    boxes, dirs = lax.axis_size("box"), lax.axis_size("dir")
    devices = boxes * dirs
    leaf_count, unknowns, samples = currents.shape
    leaf_top, directions, _ = aggregate_maps.shape
    runs = leaf_count // leaf_top
    top_local, list_slots = far_boxes.shape
    rows = directions // dirs
    plane = top_local * rows
    cut = min(rows, 16)
    group = top_local * cut
    groups = rows // cut
    chunks = leaf_top // AGG_CHUNK
    width = -(-devices * runs // 128) * 128

    held = functools.partial(pltpu.with_memory_space_constraint, memory_space=pltpu.HBM)
    hbm = pl.BlockSpec(memory_space=pltpu.HBM)
    vmem = pl.BlockSpec(memory_space=pltpu.VMEM)
    smem = pl.BlockSpec(memory_space=pltpu.SMEM)
    dma = pltpu.SemaphoreType.DMA
    incoming, near, maps = pl.pallas_call(
        functools.partial(rays_kernel, boxes, dirs, runs),
        out_shape=(
            jax.ShapeDtypeStruct((directions, runs * samples), BF16),
            jax.ShapeDtypeStruct((runs, leaf_top, unknowns, samples), BF16),
            jax.ShapeDtypeStruct(disaggregate_maps.shape, BF16),
        ),
        in_specs=[hbm] * 10,
        out_specs=(vmem, vmem, vmem),
        scratch_shapes=[
            pltpu.VMEM((leaf_count + 2, unknowns, samples), BF16),
            pltpu.VMEM((directions, runs * samples), F32),
            pltpu.VMEM((runs, directions, samples), BF16),
            pltpu.VMEM((boxes, dirs, runs, rows, samples), BF16),
            pltpu.VMEM(near_blocks.shape, BF16),
            pltpu.SMEM((2, leaf_count), jnp.int32),
            pltpu.SMEM((leaf_count,), jnp.int32),
            pltpu.VMEM((top_local, list_slots), jnp.int32),
            pltpu.SMEM((top_local,), jnp.int32),
            pltpu.VMEM((1, samples), F32),
            pltpu.VMEM((1, width), F32),
            pltpu.VMEM((devices, 1, width), F32),
            pltpu.VMEM((top_local, list_slots, 128), F32),
            pltpu.VMEM((plane, 2 * width), BF16),
            pltpu.VMEM((groups, 2 * group, width), BF16),
            pltpu.VMEM((boxes, groups, 2 * group, group), BF16),
            pltpu.VMEM((groups, 2 * group, samples), F32),
            pltpu.VMEM((2 * samples, 2 * samples), BF16),
            pltpu.VMEM((dirs, rows, runs * samples), BF16),
            pltpu.VMEM((dirs, rows, runs * samples), BF16),
            dma((chunks,)),
            dma((runs, chunks)),
            dma((7,)),
            dma,
            dma((devices,)),
            dma((devices,)),
            dma(((2 * REACH + 1) * dirs,)),
            dma((devices,)),
            dma((devices,)),
            dma((dirs,)),
            dma((dirs,)),
            dma((2,)),
            dma((2,)),
        ],
        compiler_params=pltpu.CompilerParams(
            collective_id=0, has_side_effects=True, vmem_limit_bytes=30 * 2**20
        ),
        name="rays",
    )(
        held(currents),
        held(aggregate_maps),
        held(disaggregate_maps),
        held(translate_coef),
        held(near_blocks),
        held(near_links.T),
        held(leaf_parent),
        held(far_boxes),
        held(far_counts),
        held(time_kernel.reshape(1, samples)),
    )

    chunk = 4
    out_shape = (runs, leaf_top, unknowns, samples)
    out = pl.pallas_call(
        functools.partial(field_kernel, runs, chunk),
        out_shape=jax.ShapeDtypeStruct(out_shape, BF16),
        in_specs=[vmem, vmem, vmem],
        out_specs=hbm,
        scratch_shapes=[pltpu.VMEM(out_shape, BF16), dma((leaf_top // chunk,))],
        name="field",
        compiler_params=pltpu.CompilerParams(vmem_limit_bytes=10 * 2**20),
    )(maps, incoming, near)
    return out.reshape(leaf_count, unknowns, samples)


def solution(mesh):
    return jax.shard_map(
        per_device,
        mesh=mesh,
        in_specs=(
            P(("box", "dir"), None, None),
            P(("box", "dir")),
            P(("box", "dir"), None),
            P(),
            P(),
            P("box", None),
            P("box"),
            P("box", None, None),
            P(),
            P(),
        ),
        out_specs=P(("box", "dir"), None, None),
        check_vma=False,
    )
```

```python
import functools
import jax
import jax.numpy as jnp
from jax import lax
from jax.experimental import pallas as pl
from jax.experimental.pallas import tpu as pltpu
from jax.sharding import PartitionSpec as P

MESH = pl.DeviceIdType.MESH
F32 = jnp.float32
BF16 = jnp.bfloat16
AGG_CHUNK = 4
NEAR_BLOCK = 8
REACH = 2
EARLY_BLOCKS = 3


def split_high_low(value):
    high = value.astype(BF16)
    return high, (value - high.astype(F32)).astype(BF16)


def rays_kernel(
    boxes,
    dirs,
    runs,
    cur_hbm,
    agg_hbm,
    dis_hbm,
    coef_hbm,
    blocks_hbm,
    links_hbm,
    leaf_parent_hbm,
    lists_hbm,
    counts_hbm,
    kernel_hbm,
    incoming_ref,
    near_ref,
    dis_ref,
    leaf,
    acc,
    rays,
    rays_all,
    blocks_ref,
    links_ref,
    leaf_parent_ref,
    lists_ref,
    counts_ref,
    kernel_ref,
    parent_row_ref,
    parent_all,
    coef,
    weights_ref,
    split_ref,
    spread_ref,
    far_ref,
    time_ref,
    stage_ref,
    landed,
    agg_sem,
    cur_sem,
    small_sem,
    dis_sem,
    par_send,
    par_recv,
    ray_send,
    ray_recv,
    relay_send,
    back_send,
    back_recv,
    rim_send,
    rim_recv,
):
    my_box = lax.axis_index("box")
    my_dir = lax.axis_index("dir")
    me = my_box * dirs + my_dir
    devices = boxes * dirs
    leaf_top = agg_hbm.shape[0]
    samples = cur_hbm.shape[-1]
    directions = agg_hbm.shape[1]
    rows = directions // dirs
    top_local = counts_ref.shape[0]
    slots = lists_ref.shape[1]
    width = parent_row_ref.shape[-1]
    places = dirs * runs
    group = far_ref.shape[1] // 2
    cut = group // places
    leaves = runs * leaf_top
    dot = functools.partial(jnp.dot, preferred_element_type=F32)
    peers = [(kb, kd) for kb in range(boxes) for kd in range(dirs) if kb or kd]

    def target(kb, kd):
        return lax.rem(my_box + kb, boxes), lax.rem(my_dir + kd, dirs)

    chunks = leaf_top // AGG_CHUNK

    def loads(c):
        first = c * AGG_CHUNK
        out = []
        for j in range(runs):
            at = j * leaf_top + first
            out.append(
                pltpu.make_async_copy(
                    cur_hbm.at[pl.ds(at, AGG_CHUNK)],
                    leaf.at[pl.ds(at + 1, AGG_CHUNK)],
                    cur_sem.at[j, c],
                )
            )
        out.append(
            pltpu.make_async_copy(
                agg_hbm.at[pl.ds(first, AGG_CHUNK)],
                dis_ref.at[pl.ds(first, AGG_CHUNK)],
                agg_sem.at[c],
            )
        )
        return out

    def start_loads(c, carry):
        for copy in loads(c):
            copy.start()
        return carry

    block_at = my_dir * rows
    lane_tile = lax.div(block_at, 128) * 128
    small = [
        (leaf_parent_hbm, leaf_parent_ref),
        (links_hbm, links_ref),
        (counts_hbm, counts_ref),
        (kernel_hbm, kernel_ref),
        (lists_hbm, lists_ref),
        (blocks_hbm, blocks_ref),
        (coef_hbm.at[:, :, pl.ds(pl.multiple_of(lane_tile, 128), 128)], coef),
    ]
    small = [pltpu.make_async_copy(a, b, small_sem.at[i]) for i, (a, b) in enumerate(small)]
    small[0].start()
    lax.fori_loop(0, chunks, start_loads, 0)

    barrier = pltpu.get_barrier_semaphore()
    for kb, kd in peers:
        tb, td = target(kb, kd)
        pl.semaphore_signal(
            barrier, inc=1, device_id={"box": tb, "dir": td}, device_id_type=MESH
        )

    @pl.when(me == 0)
    def _():
        leaf[0] = jnp.zeros(leaf.shape[1:], BF16)

    @pl.when(me == devices - 1)
    def _():
        leaf[leaves + 1] = jnp.zeros(leaf.shape[1:], BF16)

    small[0].wait()
    lane = lax.broadcasted_iota(jnp.int32, (1, width), 1)
    spare = jnp.where(me == 0, -1, 0)
    parent_row = jnp.where(lane >= devices * runs, spare, jnp.zeros((1, width), jnp.int32))
    for j in range(runs):
        parent_row = jnp.where(lane == me * runs + j, leaf_parent_ref[j * leaf_top], parent_row)
    parent_row_ref[...] = parent_row.astype(F32)
    parent_all[me] = parent_row.astype(F32)
    acc[...] = jnp.zeros_like(acc)

    def aggregate(c, carry):
        for copy in loads(c):
            copy.wait()
        first = c * AGG_CHUNK
        maps = jnp.concatenate([dis_ref[first + i] for i in range(AGG_CHUNK)], axis=1)
        held = jnp.concatenate(
            [
                jnp.concatenate([leaf[1 + j * leaf_top + first + i] for j in range(runs)], axis=1)
                for i in range(AGG_CHUNK)
            ],
            axis=0,
        )
        acc[...] += dot(maps, held)
        return carry

    def parent_copy(kb, kd):
        tb, td = target(kb, kd)
        return pltpu.make_async_remote_copy(
            src_ref=parent_row_ref,
            dst_ref=parent_all.at[me],
            send_sem=par_send.at[tb * dirs + td],
            recv_sem=par_recv.at[me],
            device_id={"box": tb, "dir": td},
            device_id_type=MESH,
        )

    lax.fori_loop(0, chunks - 6, aggregate, 0)
    for copy in small[1:]:
        copy.start()
    pl.semaphore_wait(barrier, len(peers))
    for kb, kd in peers:
        parent_copy(kb, kd).start()
    lax.fori_loop(chunks - 6, chunks, aggregate, 0)

    def ray_copy(delta, kd):
        tb = my_box + delta
        td = lax.rem(my_dir + kd, dirs)
        block = pl.ds(pl.multiple_of(td * rows, rows), rows)
        return pltpu.make_async_remote_copy(
            src_ref=rays.at[:, block, :],
            dst_ref=rays_all.at[my_box, my_dir],
            send_sem=ray_send.at[(delta + REACH) * dirs + td],
            recv_sem=ray_recv.at[me],
            device_id={"box": tb, "dir": td},
            device_id_type=MESH,
        )

    def relay_copy(side, away, sd):
        sb = my_box - side * away
        slot = sb * dirs + sd
        return pltpu.make_async_remote_copy(
            src_ref=rays_all.at[sb, sd],
            dst_ref=rays_all.at[sb, sd],
            send_sem=relay_send.at[slot],
            recv_sem=ray_recv.at[slot],
            device_id={"box": my_box + side, "dir": my_dir},
            device_id_type=MESH,
        )

    def rim_copy(side):
        other = lax.rem(me + (1 if side == 0 else devices - 1), devices)
        return pltpu.make_async_remote_copy(
            src_ref=cur_hbm.at[leaves - 1 if side == 0 else 0],
            dst_ref=leaf.at[0 if side == 0 else leaves + 1],
            send_sem=rim_send.at[side],
            recv_sem=rim_recv.at[side],
            device_id={"box": lax.div(other, dirs), "dir": lax.rem(other, dirs)},
            device_id_type=MESH,
        )

    def inside(box):
        return jnp.logical_and(box >= 0, box < boxes)

    def when_sending(delta, action):
        def every():
            for kd in range(dirs):
                if delta or kd:
                    action(ray_copy(delta, kd))

        if delta:
            pl.when(inside(my_box + delta))(every)
        else:
            every()

    for j in range(runs):
        rays[j] = acc[:, j * samples : (j + 1) * samples].astype(BF16)
    deltas = sorted(range(-REACH, REACH + 1), key=lambda delta: -abs(delta))
    deltas = [delta for delta in deltas if abs(delta) < boxes]
    for delta in deltas:
        when_sending(delta, lambda copy: copy.start())

    @pl.when(me < devices - 1)
    def _():
        rim_copy(0).start()

    @pl.when(me > 0)
    def _():
        rim_copy(1).start()

    own = pl.ds(pl.multiple_of(block_at, rows), rows)
    rays_all[my_box, my_dir] = rays[:, own, :]
    dis_copy = pltpu.make_async_copy(dis_hbm, dis_ref, dis_sem)
    dis_copy.start()
    for copy in small[1:]:
        copy.wait()

    def near_block(step):
        first = step * NEAR_BLOCK
        pairs = [
            jnp.concatenate([leaf[j * leaf_top + first + u] for j in range(runs)], axis=1)
            for u in range(NEAR_BLOCK + 2)
        ]
        for u in range(NEAR_BLOCK):
            mid = dot(blocks_ref[0], pairs[u + 1])
            low = dot(blocks_ref[1], pairs[u])
            high = dot(blocks_ref[2], pairs[u + 2])
            for j in range(runs):
                span = slice(j * samples, (j + 1) * samples)
                at = j * leaf_top + first + u
                with_low = links_ref[0, at].astype(F32)
                with_high = links_ref[1, at].astype(F32)
                part = mid[:, span] + with_low * low[:, span] + with_high * high[:, span]
                near_ref[j, first + u] = part.astype(BF16)

    def arrived(ref, send_sem, recv_sem):
        pltpu.make_async_remote_copy(
            src_ref=ref,
            dst_ref=ref,
            send_sem=send_sem,
            recv_sem=recv_sem,
            device_id={"box": my_box, "dir": lax.rem(my_dir + 1, dirs)},
            device_id_type=MESH,
        ).wait_recv()

    def ray_arrived(sb, sd):
        slot = sb * dirs + sd
        arrived(rays_all.at[sb, sd], relay_send.at[slot], ray_recv.at[slot])

    def each_relay(action):
        for away in range(REACH, boxes - 1):
            for side in (1, -1):
                fits = jnp.logical_and(inside(my_box - side * away), inside(my_box + side))
                pl.when(fits)(functools.partial(action, side, away))

    blocks = leaf_top // NEAR_BLOCK
    late_blocks = blocks - 2 - EARLY_BLOCKS
    per_step = dirs // (late_blocks + 1)

    def near_only(step, carry):
        near_block(step)
        return carry

    def relay(side, away, i, carry):
        sd = lax.rem(my_dir - i + dirs, dirs)
        ray_arrived(my_box - side * away, sd)
        relay_copy(side, away, sd).start()
        return carry

    def relay_span(first, last):
        def some(side, away):
            lax.fori_loop(first, last, functools.partial(relay, side, away), 0)

        each_relay(some)

    def near_relay(step, carry):
        near_block(step)
        first = (step - EARLY_BLOCKS - 1) * per_step
        relay_span(first, first + per_step)
        return carry

    lax.fori_loop(1, 1 + EARLY_BLOCKS, near_only, 0)
    lax.fori_loop(1 + EARLY_BLOCKS, blocks - 1, near_relay, 0)
    relay_span(late_blocks * per_step, dirs)

    spread_time = pltpu.roll(
        jnp.broadcast_to(kernel_ref[...], (samples, samples)), 0, 1, stride=1, stride_axis=0
    )
    causal = lax.broadcasted_iota(jnp.int32, (samples, samples), 1) >= lax.broadcasted_iota(
        jnp.int32, (samples, samples), 0
    )
    time_high, time_low = split_high_low(jnp.where(causal, spread_time, 0.0))
    time_ref[:samples, :samples] = time_high
    time_ref[:samples, samples:] = time_low
    time_ref[samples:, :samples] = time_high
    time_ref[samples:, samples:] = jnp.zeros_like(time_low)

    for kb, kd in peers:
        sb, sd = target(kb, kd)
        slot = sb * dirs + sd
        arrived(parent_all.at[slot], par_send.at[slot], par_recv.at[slot])
    parents = jnp.zeros((1, width), F32)
    for slot in range(devices):
        parents = parents + parent_all[slot]
    column = jnp.broadcast_to(parents, (128, width)).T[:, :slots]
    spot = lax.broadcasted_iota(jnp.int32, (1, slots), 1)
    turn = lax.rem(128 - (block_at - lane_tile), 128)
    for c in range(top_local):
        used = jnp.where(spot < counts_ref[c], lists_ref[c : c + 1, :], -2)
        match = (column == used.astype(F32)).astype(F32).astype(BF16)
        high, low = split_high_low(pltpu.roll(coef[c], turn, 1)[:, :rows])
        both = lax.dot_general(
            jnp.concatenate([high, low], axis=1),
            match,
            (((0,), (1,)), ((), ())),
            preferred_element_type=F32,
        )
        high, low = split_high_low(both[:rows, :] + both[rows:, :])
        weights_ref[c * rows : (c + 1) * rows, :width] = high
        weights_ref[c * rows : (c + 1) * rows, width:] = low

    def iota(shape, axis):
        return lax.broadcasted_iota(jnp.int32, shape, axis)

    total = places * rows
    for g in range(total // group):
        place = lax.div(iota((group, width), 0), cut)
        here = iota((group, width), 1) == my_box * places + place
        parent = jnp.sum(jnp.where(here, parents, 0.0), axis=1, keepdims=True)
        shape = (group, total)
        owner = (my_box * top_local + lax.div(iota(shape, 1), rows)).astype(F32)
        same = lax.rem(iota(shape, 1), rows) == g * cut + lax.rem(iota(shape, 0), cut)
        pick = jnp.where(jnp.logical_and(parent == owner, same), 1.0, 0.0).astype(BF16)
        moved = dot(pick, weights_ref[...]).astype(BF16)
        split_ref[g, :group, :] = moved[:, :width]
        split_ref[g, group:, :] = moved[:, width:]

    def spread(b, carry):
        shape = (width, group)
        pick = iota(shape, 0) == b * places + lax.div(iota(shape, 1), cut)
        pick = jnp.where(pick, 1.0, 0.0).astype(BF16)
        shape = (2 * group, group)
        same = lax.rem(iota(shape, 0), cut) == lax.rem(iota(shape, 1), cut)
        for g in range(total // group):
            spread_ref[b, g] = jnp.where(same, dot(split_ref[g], pick), 0.0).astype(BF16)
        return carry

    lax.fori_loop(0, boxes, spread, 0)
    half = lax.div(my_box * 2, boxes)
    for n in range(boxes):
        sb = lax.rem(my_box + n * (1 - 2 * half) + boxes, boxes)

        def plain():
            for kd in range(1 if n == 0 else 0, dirs):
                ray_arrived(sb, lax.rem(my_dir + kd, dirs))

        if n == 0:
            plain()
        else:
            up = jnp.logical_and(sb <= my_box - REACH, my_box + 1 < boxes)
            down = jnp.logical_and(sb >= my_box + REACH, my_box >= 1)
            pl.when(jnp.logical_not(jnp.logical_or(up, down)))(plain)
        for g in range(total // group):
            held = rays_all[sb, :, :, g * cut : (g + 1) * cut, :].reshape(group, samples)
            part_sum = dot(spread_ref[sb, g], held)
            if n == 0:
                far_ref[g] = part_sum
            else:
                far_ref[g] += part_sum

    for g in range(total // group):
        high, low = split_high_low(far_ref[g, :group, :] + far_ref[g, group:, :])
        both = dot(jnp.concatenate([high, low], axis=1), time_ref[...])
        incoming = (both[:, :samples] + both[:, samples:]).astype(BF16)
        for d in range(dirs):
            for j in range(runs):
                place = d * runs + j
                stage_ref[d, g * cut : (g + 1) * cut, j * samples : (j + 1) * samples] = incoming[
                    place * cut : (place + 1) * cut, :
                ]

    def back_copy(kd):
        td = lax.rem(my_dir + kd, dirs)
        return pltpu.make_async_remote_copy(
            src_ref=stage_ref.at[td],
            dst_ref=landed.at[my_dir],
            send_sem=back_send.at[td],
            recv_sem=back_recv.at[my_dir],
            device_id={"box": my_box, "dir": td},
            device_id_type=MESH,
        )

    for kd in range(1, dirs):
        back_copy(kd).start()
    landed[my_dir] = stage_ref[my_dir]

    @pl.when(me < devices - 1)
    def _():
        rim_copy(0).wait_send()
        rim_copy(1).wait_recv()

    @pl.when(me > 0)
    def _():
        rim_copy(1).wait_send()
        rim_copy(0).wait_recv()

    def last_block(step, carry):
        near_block(step * (blocks - 1))
        return carry

    lax.fori_loop(0, 2, last_block, 0)
    for kb, kd in peers:
        parent_copy(kb, kd).wait_send()
    for delta in deltas:
        when_sending(delta, lambda copy: copy.wait_send())

    def relayed(side, away):
        for sd in range(dirs):
            relay_copy(side, away, sd).wait_send()

    each_relay(relayed)
    dis_copy.wait()
    for kd in range(1, dirs):
        sd = lax.rem(my_dir + kd, dirs)
        arrived(landed.at[sd], back_send.at[sd], back_recv.at[sd])
    incoming_ref[...] = landed[...].reshape(directions, runs * samples)
    for kd in range(1, dirs):
        back_copy(kd).wait_send()


def field_kernel(runs, chunk, maps_ref, incoming_ref, near_ref, out_ref, held_out, sem):
    leaf_top, _, _ = maps_ref.shape
    samples = near_ref.shape[-1]
    held = incoming_ref[...]

    def copy(step):
        span = pl.ds(step * chunk, chunk)
        return pltpu.make_async_copy(held_out.at[:, span], out_ref.at[:, span], sem.at[step])

    def step_of(step, carry):
        for i in range(chunk):
            at = step * chunk + i
            total = jnp.dot(maps_ref[at], held, preferred_element_type=F32)
            for j in range(runs):
                part = total[:, j * samples : (j + 1) * samples]
                held_out[j, at] = (part + near_ref[j, at].astype(F32)).astype(BF16)
        copy(step).start()
        return carry

    def finish(step, carry):
        copy(step).wait()
        return carry

    steps = leaf_top // chunk
    lax.fori_loop(0, steps, step_of, 0, unroll=16)
    lax.fori_loop(0, steps, finish, 0)


def per_device(
    currents,
    leaf_parent,
    near_links,
    near_blocks,
    aggregate_maps,
    far_boxes,
    far_counts,
    translate_coef,
    time_kernel,
    disaggregate_maps,
):
    boxes, dirs = lax.axis_size("box"), lax.axis_size("dir")
    devices = boxes * dirs
    leaf_count, unknowns, samples = currents.shape
    leaf_top, directions, _ = aggregate_maps.shape
    runs = leaf_count // leaf_top
    top_local, list_slots = far_boxes.shape
    rows = directions // dirs
    plane = top_local * rows
    cut = min(rows, 16)
    group = top_local * cut
    groups = rows // cut
    chunks = leaf_top // AGG_CHUNK
    width = -(-devices * runs // 128) * 128

    held = functools.partial(pltpu.with_memory_space_constraint, memory_space=pltpu.HBM)
    hbm = pl.BlockSpec(memory_space=pltpu.HBM)
    vmem = pl.BlockSpec(memory_space=pltpu.VMEM)
    smem = pl.BlockSpec(memory_space=pltpu.SMEM)
    dma = pltpu.SemaphoreType.DMA
    incoming, near, maps = pl.pallas_call(
        functools.partial(rays_kernel, boxes, dirs, runs),
        out_shape=(
            jax.ShapeDtypeStruct((directions, runs * samples), BF16),
            jax.ShapeDtypeStruct((runs, leaf_top, unknowns, samples), BF16),
            jax.ShapeDtypeStruct(disaggregate_maps.shape, BF16),
        ),
        in_specs=[hbm] * 10,
        out_specs=(vmem, vmem, vmem),
        scratch_shapes=[
            pltpu.VMEM((leaf_count + 2, unknowns, samples), BF16),
            pltpu.VMEM((directions, runs * samples), F32),
            pltpu.VMEM((runs, directions, samples), BF16),
            pltpu.VMEM((boxes, dirs, runs, rows, samples), BF16),
            pltpu.VMEM(near_blocks.shape, BF16),
            pltpu.SMEM((2, leaf_count), jnp.int32),
            pltpu.SMEM((leaf_count,), jnp.int32),
            pltpu.VMEM((top_local, list_slots), jnp.int32),
            pltpu.SMEM((top_local,), jnp.int32),
            pltpu.VMEM((1, samples), F32),
            pltpu.VMEM((1, width), F32),
            pltpu.VMEM((devices, 1, width), F32),
            pltpu.VMEM((top_local, list_slots, 128), F32),
            pltpu.VMEM((plane, 2 * width), BF16),
            pltpu.VMEM((groups, 2 * group, width), BF16),
            pltpu.VMEM((boxes, groups, 2 * group, group), BF16),
            pltpu.VMEM((groups, 2 * group, samples), F32),
            pltpu.VMEM((2 * samples, 2 * samples), BF16),
            pltpu.VMEM((dirs, rows, runs * samples), BF16),
            pltpu.VMEM((dirs, rows, runs * samples), BF16),
            dma((chunks,)),
            dma((runs, chunks)),
            dma((7,)),
            dma,
            dma((devices,)),
            dma((devices,)),
            dma(((2 * REACH + 1) * dirs,)),
            dma((devices,)),
            dma((devices,)),
            dma((dirs,)),
            dma((dirs,)),
            dma((2,)),
            dma((2,)),
        ],
        compiler_params=pltpu.CompilerParams(
            collective_id=0, has_side_effects=True, vmem_limit_bytes=30 * 2**20
        ),
        name="rays",
    )(
        held(currents),
        held(aggregate_maps),
        held(disaggregate_maps),
        held(translate_coef),
        held(near_blocks),
        held(near_links.T),
        held(leaf_parent),
        held(far_boxes),
        held(far_counts),
        held(time_kernel.reshape(1, samples)),
    )

    chunk = 2
    out_shape = (runs, leaf_top, unknowns, samples)
    out = pl.pallas_call(
        functools.partial(field_kernel, runs, chunk),
        out_shape=jax.ShapeDtypeStruct(out_shape, BF16),
        in_specs=[vmem, vmem, vmem],
        out_specs=hbm,
        scratch_shapes=[pltpu.VMEM(out_shape, BF16), dma((leaf_top // chunk,))],
        name="field",
        compiler_params=pltpu.CompilerParams(vmem_limit_bytes=10 * 2**20),
    )(maps, incoming, near)
    return out.reshape(leaf_count, unknowns, samples)


def solution(mesh):
    return jax.shard_map(
        per_device,
        mesh=mesh,
        in_specs=(
            P(("box", "dir"), None, None),
            P(("box", "dir")),
            P(("box", "dir"), None),
            P(),
            P(),
            P("box", None),
            P("box"),
            P("box", None, None),
            P(),
            P(),
        ),
        out_specs=P(("box", "dir"), None, None),
        check_vma=False,
    )
```
